32 devices in a mesh: ex: 4 (over y, x), ey: 2 (over core), tp: 4 (over z).
Axes of the slice: x: 2, y: 2, z: 4, core: 2. Of those that a mesh axis runs over, the one named last changes fastest.
Arguments:
- tokens: bfloat16 [256, 7168], P(('ex', 'ey'), 'tp'), may hold values from -6 to 6
- cotangent: bfloat16 [256, 7168], P(('ex', 'ey'), 'tp'), may hold values from -0.59765625 to 0.59765625
- gates: bfloat16 [256, 8], P(('ex', 'ey')), may hold values from 0.049804688 to 1
- expert_ids: int32 [256, 8], P(('ex', 'ey')), may hold values from 0 to 31, all different within a row; in each aligned block of 32 rows (0 to 31, 32 to 63, ...) at most 10 rows name the same one
- saved_gate: bfloat16 [1024, 32, 80], P(None, ('ex', 'ey')), may hold values from -6 to 6
- saved_up: bfloat16 [1024, 32, 80], P(None, ('ex', 'ey')), may hold values from -6 to 6
- w_gate: bfloat16 [32, 7168, 1024], P(('ex', 'ey'), 'tp'), may hold values from -0.1875 to 0.1875
- w_up: bfloat16 [32, 7168, 1024], P(('ex', 'ey'), 'tp'), may hold values from -0.1875 to 0.1875
- w_down: bfloat16 [32, 1024, 7168], P(('ex', 'ey'), None, 'tp'), may hold values from -0.25 to 0.25
Outputs:
- grad_tokens: bfloat16 [256, 7168], P(('ex', 'ey'), 'tp')
- grad_gates: bfloat16 [256, 8], P(('ex', 'ey'))
- grad_w_gate: bfloat16 [32, 7168, 1024], P(('ex', 'ey'), 'tp')
- grad_w_up: bfloat16 [32, 7168, 1024], P(('ex', 'ey'), 'tp')
- grad_w_down: bfloat16 [32, 1024, 7168], P(('ex', 'ey'), None, 'tp')
The draws below stay inside these ranges and needn't reach their ends.
Inputs may be any that keep to these rules, and one draw needn't show every extreme that they name: `expert_ids`: each row names 8 different experts. The rows of one token group name any one expert at most 10 times, a bound that some block reaches.
All inputs are finite; a program needn't handle non-finite values.
Results may differ from the reference program's by a relative error of at most 0.025.
Values may be sent and summed in bfloat16 or wider, within the bound.
A program may use at most 128 MiB of HBM per device.

```python
import math
import jax
import jax.numpy as jnp
import numpy as np
from jax import lax

D = 7168
FF = 1024
EXPERTS = 32
TOP = 8
TOK_DEV = 32
CAP = 10
SLOTS = 80
TOKENS = 256
N_EX = 4
N_EY = 2
N_TP = 4


def spiked(entries, rng, source, target, blocks, factor):
    owner, partner = [(jnp.arange(entries.shape[dim]) // (entries.shape[dim] // blocks)).reshape([-1 if axis == dim else 1 for axis in range(entries.ndim)]) for dim in (source, target)]
    chosen = jax.random.permutation(rng, blocks)[partner]
    strong = (owner == chosen) | (owner == (partner + blocks // 2) % blocks)
    return jnp.where(strong, factor * entries, entries)


def levels(stream_key, shape, shards, low, high):
    gain, own = 1.0, jax.random.fold_in(stream_key, 6)
    for dim, parts in shards:
        draws = jnp.exp(jax.random.uniform(jax.random.fold_in(own, dim), (parts,), jnp.float32, low / len(shards), high / len(shards)))
        gain = gain * jnp.repeat(draws, shape[dim] // parts).reshape([-1 if axis == dim else 1 for axis in range(len(shape))])
    return gain


def assign_block(own_key, own, number, rows, count, top, most, skew):
    ranking = jax.random.permutation(own_key, count)
    heavy_load, usual = shares(count, rows * top, most, skew, True), shares(count, rows * top, most, skew, False)
    places = jnp.arange(count)

    def named(lengths, rotation):
        used = int((lengths > 0).sum())
        fixed = max(1, used // 4)
        moved = fixed + (places - fixed + rotation * (used - fixed)) % max(1, count - fixed)
        return jnp.zeros((count,), jnp.int32).at[ranking[jnp.where(places < fixed, places, moved)]].set(jnp.asarray(lengths, jnp.int32))

    lengths = jnp.where(number % 4 == 0, named(heavy_load, number // 4), named(usual, number - number // 4 - 1))
    mixed = jax.random.permutation(jax.random.fold_in(own, 3), count)
    donor, receiver = mixed[0:count // 2 * 2:2], mixed[1:count // 2 * 2:2]
    room = jnp.minimum(lengths[donor] - 1, most - lengths[receiver]) // 2
    room = jnp.where((donor == ranking[0]) | (receiver == ranking[0]) | (lengths[receiver] == 0), 0, jnp.maximum(room, 0))
    moved = jax.random.randint(jax.random.fold_in(own, 4), (count // 2,), 0, 1 << 20) % (room + 1)
    lengths = lengths.at[donor].add(-moved).at[receiver].add(moved)
    labels = jnp.searchsorted(jnp.cumsum(lengths), jnp.arange(rows * top), side="right").astype(jnp.int32)
    table = labels.reshape(top, rows).T
    table = table[jax.random.permutation(jax.random.fold_in(own, 1), rows)]
    rotation = jax.random.randint(jax.random.fold_in(own, 2), (rows, 1), 0, top)
    return jnp.take_along_axis(table, (jnp.arange(top)[None, :] + rotation) % top, axis=1)


def shares(count, total, most, skew, full):
    weights = [(1 << 20) // math.isqrt(standing ** skew) + 1 for standing in range(1, count + 1)]
    largest = most if full else min(most, max(-(-total // count), total * weights[0] // sum(weights)))
    least = 1 if total - largest >= count - 1 else 0
    holding, spare = [largest] + [least] * (count - 1), total - largest - least * (count - 1)
    while spare > 0:
        candidates = [i for i in range(1, count) if holding[i] < largest] or [i for i in range(1, count) if holding[i] < most]
        mass, budget = sum([weights[i] for i in candidates]), spare
        for i in candidates:
            addition = min(most - holding[i], max(1, budget * weights[i] // mass), spare)
            holding[i] = holding[i] + addition
            spare = spare - addition
    return np.array(holding)


def centred(stream_key, shape, deviation, limit, shards=(), kind=jnp.bfloat16):
    entries = jax.random.normal(stream_key, shape, jnp.float32) * deviation
    if len(shards) > 0:
        entries = levels(stream_key, shape, shards, -0.22, 0.18) * entries
    return jnp.clip(entries, min=-limit, max=limit).astype(kind)


def heavy_noise(key, shape, scale, limit, cuts, heavy, held_as=jnp.bfloat16):
    result = scale * jax.random.normal(key, shape, jnp.float32)
    if cuts:
        result = result * levels(key, shape, cuts, -0.22, 0.18)
    return jnp.clip(spiked(result, jax.random.fold_in(key, 3), *heavy), -limit, limit).astype(held_as)


def setup_inputs(seed: int = 0) -> dict:
    splits = jax.random.split(jax.random.key(seed), 10)
    tokens = centred(splits[0], (TOKENS, D), 1.0, 6.0, ((0, 8), (1, 4)))
    cotangent = centred(splits[1], (TOKENS, D), 0.1, 0.59765625, ((0, 8), (1, 4)))
    gates = jnp.clip(jnp.exp(math.log(1.0) - 2.9996462 * jax.random.uniform(splits[2], (TOKENS, TOP), jnp.float32) ** levels(splits[2], (TOKENS, TOP), ((0, 8),), -0.2, 0.2)), 0.049804688, 1.0).astype(jnp.bfloat16)
    expert_ids_keys = jax.random.split(jax.random.fold_in(splits[3], 1), TOKENS // TOK_DEV)
    expert_ids_turns = jax.random.permutation(jax.random.fold_in(splits[3], 3), TOKENS // TOK_DEV)
    expert_ids = jax.vmap(lambda own, number: assign_block(jax.random.fold_in(splits[3], 2), own, number, TOK_DEV, EXPERTS, TOP, CAP, 0))(expert_ids_keys, expert_ids_turns).reshape((TOKENS, TOP))
    saved_gate = centred(splits[4], (FF, EXPERTS, SLOTS), 1.0, 6.0, ((1, 8),))
    saved_up = centred(splits[5], (FF, EXPERTS, SLOTS), 1.0, 6.0, ((1, 8),))
    w_gate = centred(splits[6], (EXPERTS, D, FF), FF ** -0.5, 0.1875, ((0, 8), (1, 4)))
    w_up = centred(splits[7], (EXPERTS, D, FF), FF ** -0.5, 0.1875, ((0, 8), (1, 4)))
    w_down = heavy_noise(splits[8], (EXPERTS, FF, D), FF ** -0.5, 0.25, ((0, 8), (2, 4)), (2, 1, 4, 2.0))
    return {"tokens": tokens, "cotangent": cotangent, "gates": gates, "expert_ids": expert_ids, "saved_gate": saved_gate, "saved_up": saved_up, "w_gate": w_gate, "w_up": w_up, "w_down": w_down}


def slot_codes(expert_ids, capacity, expert_count):
    tok_rows, top_count = expert_ids.shape
    flat = expert_ids.reshape(-1)
    onehot = (flat[:, None] == jnp.arange(expert_count, dtype=jnp.int32)[None, :]).astype(jnp.int32)
    before = jnp.cumsum(onehot, axis=0) - onehot
    position = jnp.sum(before * onehot, axis=1)
    return (flat * capacity + position).reshape(tok_rows, top_count)


def reference(tokens, cotangent, gates, expert_ids, saved_gate, saved_up, w_gate, w_up, w_down):
    source_count = N_EX * N_EY
    slot_total = source_count * CAP
    block_width = D // N_TP
    blocks = expert_ids.reshape(source_count, TOK_DEV, TOP)
    codes = jax.vmap(lambda stretch_ids: slot_codes(stretch_ids, CAP, EXPERTS))(blocks)
    position = codes - blocks * CAP
    source = jnp.arange(source_count, dtype=jnp.int32)[:, None, None]
    row_id = (blocks * slot_total + source * CAP + position).reshape(TOKENS, TOP).astype(jnp.int32)
    pair_index = jnp.arange(TOKENS * TOP, dtype=jnp.int32)
    table = jnp.full((EXPERTS * slot_total,), TOKENS * TOP, jnp.int32).at[row_id.reshape(-1)].set(pair_index)
    table = table.reshape(EXPERTS, slot_total)
    x_pad = jnp.concatenate([tokens, jnp.zeros((1, D), tokens.dtype)], axis=0)
    dy_pad = jnp.concatenate([cotangent, jnp.zeros((1, D), cotangent.dtype)], axis=0)
    g_pad = jnp.concatenate([gates.reshape(-1), jnp.zeros((1,), gates.dtype)], axis=0)
    gate_major = jnp.moveaxis(saved_gate, 1, 0)
    up_major = jnp.moveaxis(saved_up, 1, 0)

    def one_expert(bundle):
        pairs, weight_gate, weight_up, weight_down, gate_pre, up_pre = bundle
        token_row = pairs // TOP
        x_rows = x_pad[token_row]
        dy_rows = dy_pad[token_row]
        g_rows = g_pad[pairs]
        scaled = (g_rows.astype(jnp.float32)[:, None] * dy_rows.astype(jnp.float32)).astype(jnp.bfloat16)
        act_gate = gate_pre.astype(jnp.float32)
        act_up = up_pre.astype(jnp.float32)
        sigm = jax.nn.sigmoid(act_gate)
        hidden = (act_gate * sigm * act_up).astype(jnp.bfloat16)
        out_rows = lax.dot_general(hidden, weight_down, (((0,), (0,)), ((), ())), preferred_element_type=jnp.float32)
        prod = (dy_rows.astype(jnp.float32) * out_rows).reshape(slot_total, N_TP, block_width)
        score_part = lax.optimization_barrier(jnp.sum(prod, axis=2).astype(jnp.bfloat16))
        score = jnp.sum(score_part.astype(jnp.float32), axis=1).astype(jnp.bfloat16)
        down_blocks = weight_down.astype(jnp.float32).reshape(FF, N_TP, block_width)
        scaled_blocks = scaled.astype(jnp.float32).reshape(slot_total, N_TP, block_width)
        dh_part = jnp.einsum("fjd,sjd->jfs", down_blocks, scaled_blocks, precision=lax.Precision.HIGHEST)
        dh_part = lax.optimization_barrier(dh_part.astype(jnp.bfloat16))
        dh_sum = jnp.sum(dh_part.astype(jnp.float32), axis=0).astype(jnp.bfloat16)
        dh_wide = dh_sum.astype(jnp.float32)
        d_gate_pre = (dh_wide * act_up * sigm * (1.0 + act_gate * (1.0 - sigm))).astype(jnp.bfloat16)
        d_up_pre = (dh_wide * act_gate * sigm).astype(jnp.bfloat16)
        dims = (((0,), (1,)), ((), ()))
        dx_rows = lax.dot_general(d_gate_pre, weight_gate, dims, preferred_element_type=jnp.float32)
        dx_rows = dx_rows + lax.dot_general(d_up_pre, weight_up, dims, preferred_element_type=jnp.float32)
        grad_gate_w = lax.dot_general(x_rows, d_gate_pre, dims, preferred_element_type=jnp.float32)
        grad_up_w = lax.dot_general(x_rows, d_up_pre, dims, preferred_element_type=jnp.float32)
        grad_down_w = jnp.dot(hidden, scaled, preferred_element_type=jnp.float32)
        return (dx_rows.astype(jnp.bfloat16), score, grad_gate_w.astype(jnp.bfloat16),
                grad_up_w.astype(jnp.bfloat16), grad_down_w.astype(jnp.bfloat16))

    dx_all, score_all, grad_w_gate, grad_w_up, grad_w_down = lax.map(
        one_expert, (table, w_gate, w_up, w_down, gate_major, up_major))
    dx_flat = dx_all.reshape(EXPERTS * slot_total, D)
    total = jnp.zeros((TOKENS, D), jnp.float32)
    for choice_index in range(TOP):
        total = total + dx_flat[row_id[:, choice_index]].astype(jnp.float32)
    grad_tokens = total.astype(jnp.bfloat16)
    grad_gates = score_all.reshape(-1)[row_id]
    return grad_tokens, grad_gates, grad_w_gate, grad_w_up, grad_w_down
```

```python
import functools
import jax
import jax.numpy as jnp
from jax import lax
from jax.experimental import pallas as pl
from jax.experimental.pallas import tpu as pltpu
from jax.sharding import PartitionSpec as P

LANES = 128
GROUP = ("ex", "ey")


def scatter_blocks(blocks, parts):
    if parts > 4:
        got = lax.all_to_all(blocks, "tp", split_axis=0, concat_axis=0, tiled=True)
        return [got[i] for i in range(parts)]
    me = lax.axis_index("tp")
    got = [lax.dynamic_index_in_dim(blocks, me, 0, keepdims=False)]
    for step in range(1, parts):
        piece = lax.dynamic_index_in_dim(blocks, (me + step) % parts, 0, keepdims=False)
        got.append(lax.ppermute(piece, "tp", [(i, (i + step) % parts) for i in range(parts)]))
    return got


def block_sum(terms):
    return sum(term.astype(jnp.float32) for term in terms).astype(jnp.bfloat16)


def gather_pieces(block, parts):
    if parts > 4:
        return [lax.all_gather(block, "tp", axis=0)]
    shifts = [[(i, (i + step) % parts) for i in range(parts)] for step in range(1, parts)]
    return [block] + [lax.ppermute(block, "tp", shift) for shift in shifts]


def in_order(pieces, parts):
    if parts > 4:
        return pieces[0]
    me = lax.axis_index("tp")
    whole = jnp.zeros((parts,) + pieces[0].shape, pieces[0].dtype)
    for step, piece in enumerate(pieces):
        whole = lax.dynamic_update_index_in_dim(whole, piece, (me - step) % parts, 0)
    return whole


def on_device_plain(tokens, cotangent, gates, expert_ids, saved_gate, saved_up, w_gate, w_up, w_down):
    groups = lax.axis_size(GROUP)
    parts = lax.axis_size("tp")
    rows, width = tokens.shape
    top = expert_ids.shape[1]
    hidden_units, local, slots = saved_gate.shape
    capacity = slots // groups
    total = groups * rows
    first = lax.axis_index(GROUP) * local

    extra = jnp.concatenate(
        [gates, expert_ids.astype(jnp.bfloat16), jnp.zeros((rows, LANES - 2 * top), jnp.bfloat16)],
        axis=1,
    )
    packed = jnp.concatenate([cotangent, extra], axis=1)
    packed = lax.all_gather(packed, GROUP, axis=0, tiled=True)
    tokens, packed = lax.optimization_barrier((tokens, packed))
    all_x = lax.all_to_all(
        jnp.broadcast_to(tokens[None], (groups, rows, width)),
        GROUP, split_axis=0, concat_axis=0, tiled=True,
    ).reshape(total, width)
    all_dy = packed[:, :width]
    small = packed[:, width:].astype(jnp.float32).T
    all_gates = small[:top]
    all_ids = small[top : 2 * top].astype(jnp.int32)

    match = all_ids[None] == first + jnp.arange(local, dtype=jnp.int32)[:, None, None]
    named = jnp.sum(match.astype(jnp.float32), axis=1)
    gate_of = jnp.sum(jnp.where(match, all_gates[None], 0.0), axis=1)
    place = jnp.arange(total, dtype=jnp.int32)
    group_of = place // rows
    earlier = (place[:, None] < place[None, :]) & (group_of[:, None] == group_of[None, :])
    position = jnp.dot(
        named.astype(jnp.bfloat16), earlier.astype(jnp.bfloat16), preferred_element_type=jnp.float32
    ).astype(jnp.int32)
    row_of = jnp.where(named > 0, group_of[None] * capacity + position, -1)
    taken = row_of[:, None, :] == jnp.arange(slots, dtype=jnp.int32)[None, :, None]
    chosen = taken.astype(jnp.bfloat16).reshape(local * slots, total)
    gate_rows = jnp.sum(jnp.where(taken, gate_of[:, None, :], 0.0), axis=2, keepdims=True)

    dy_rows = jnp.dot(chosen, all_dy, preferred_element_type=jnp.float32).astype(jnp.bfloat16)
    dy_rows = dy_rows.reshape(local, slots, width)
    halves = 2 if local % 2 == 0 else 1
    each = local // halves
    cuts = [slice(h * each, (h + 1) * each) for h in range(halves)]
    received = []
    for cut in cuts:
        raw = jnp.einsum(
            "erd,efd->erf", dy_rows[cut], w_down[cut], preferred_element_type=jnp.float32
        ).astype(jnp.bfloat16)
        raw = raw.reshape(parts, each * slots // parts, hidden_units)
        received.append(scatter_blocks(raw, parts))

    scaled = (gate_rows * dy_rows.astype(jnp.float32)).astype(jnp.bfloat16)
    act_gate = saved_gate.transpose(1, 2, 0).astype(jnp.float32)
    act_up = saved_up.transpose(1, 2, 0).astype(jnp.float32)
    sigm = jax.nn.sigmoid(act_gate)
    hidden = (act_gate * sigm * act_up).astype(jnp.bfloat16)
    sums = [block_sum(received[0])]
    hidden, scaled, sums[0] = lax.optimization_barrier((hidden, scaled, sums[0]))
    grad_w_down = jnp.einsum(
        "erf,erd->efd", hidden, scaled, preferred_element_type=jnp.float32
    ).astype(jnp.bfloat16)

    for terms in received[1:]:
        terms, grad_w_down = lax.optimization_barrier((terms, grad_w_down))
        sums.append(block_sum(terms))
    gathered = [gather_pieces(block, parts) for block in sums]
    d_gate, d_up, score, dx_rows = [], [], [], []
    for cut, pieces in zip(cuts, gathered):
        if dx_rows:
            pieces, dx_rows[-1] = lax.optimization_barrier((pieces, dx_rows[-1]))
        raw = in_order(pieces, parts).reshape(each, slots, hidden_units).astype(jnp.float32)
        a, u, q = act_gate[cut], act_up[cut], sigm[cut]
        dh = gate_rows[cut] * raw
        part_score = jnp.sum(raw * hidden[cut].astype(jnp.float32), axis=2, keepdims=True)
        part_gate = (dh * u * q * (1.0 + a * (1.0 - q))).astype(jnp.bfloat16)
        part_up = (dh * a * q).astype(jnp.bfloat16)
        part_gate, part_up = lax.optimization_barrier((part_gate, part_up))
        dx = jnp.einsum("erf,edf->erd", part_gate, w_gate[cut], preferred_element_type=jnp.float32)
        dx = dx + jnp.einsum("erf,edf->erd", part_up, w_up[cut], preferred_element_type=jnp.float32)
        dx_rows.append(dx.astype(jnp.bfloat16))
        d_gate.append(part_gate)
        d_up.append(part_up)
        score.append(part_score)
    d_gate, d_up, score, dx_rows = [
        jnp.concatenate(pieces, axis=0) for pieces in (d_gate, d_up, score, dx_rows)
    ]
    dx_rows = dx_rows.reshape(local * slots, width)
    own = jnp.arange(LANES)[None, None, :] == jnp.arange(local)[:, None, None]
    score_cols = jnp.where(own, score, 0.0).astype(jnp.bfloat16).reshape(local * slots, LANES)
    over_rows = (((0,), (0,)), ((), ()))
    back = [
        lax.dot_general(chosen, part, over_rows, preferred_element_type=jnp.float32).astype(
            jnp.bfloat16
        )
        for part in (dx_rows, score_cols)
    ]
    back = jnp.concatenate(back, axis=1).reshape(groups, rows, width + LANES)
    back = lax.all_to_all(back, GROUP, split_axis=0, concat_axis=0, tiled=True)

    x_rows = jnp.dot(chosen, all_x, preferred_element_type=jnp.float32).astype(jnp.bfloat16)
    x_rows = x_rows.reshape(local, slots, width)
    grad_w_gate = jnp.einsum(
        "erd,erf->edf", x_rows, d_gate, preferred_element_type=jnp.float32
    ).astype(jnp.bfloat16)
    grad_w_up = jnp.einsum(
        "erd,erf->edf", x_rows, d_up, preferred_element_type=jnp.float32
    ).astype(jnp.bfloat16)

    grad_tokens = jnp.sum(back[:, :, :width].astype(jnp.float32), axis=0).astype(jnp.bfloat16)
    table = back[:, :, width : width + local].transpose(1, 0, 2).reshape(rows, groups * local)
    picks = expert_ids[:, :, None] == jnp.arange(groups * local, dtype=jnp.int32)[None, None, :]
    grad_gates = jnp.sum(
        jnp.where(picks, table.astype(jnp.float32)[:, None, :], 0.0), axis=2
    ).astype(jnp.bfloat16)
    return (grad_tokens, grad_gates, grad_w_gate, grad_w_up, grad_w_down)


MESH = pl.DeviceIdType.MESH
HALVES = 2
LAG = 2
NT = (((1,), (1,)), ((), ()))


def mm(a, b):
    return jnp.dot(a, b, preferred_element_type=jnp.float32)


def mm_dims(a, b, dims):
    return lax.dot_general(a, b, dims, preferred_element_type=jnp.float32)


def exchange_kernel(
    cap,
    gates_in, ids_in, cot, tok, act_gate, act_up, w_gate, w_up, w_down,
    x_cols_out, scaled_out, hidden_out, d_gate_out, d_up_out, back_out,
    small, dy_all, x_all, sm_all, wd, wg, wu, chosen, chosen_t, gate_rows,
    x_cols, scaled, hidden_t, hidden, d_gate, d_up, back, to_gate, to_up,
    own, from_end, pair, from_mid, total, dx_acc, back_acc, score_acc, score_cols,
    w_sem, out_sem, dy_send, dy_recv, x_send, x_recv, sm_send, sm_recv,
    end_send, end_recv, mid_send, mid_recv, tot_send, tot_recv,
):
    ex, ey, tp = lax.axis_index("ex"), lax.axis_index("ey"), lax.axis_index("tp")
    n_ex, n_ey = lax.axis_size("ex"), lax.axis_size("ey")
    n_tp = lax.axis_size("tp")
    groups = n_ex * n_ey
    group = ex * n_ey + ey
    rows, width = cot.shape
    top = gates_in.shape[0]
    local, slots, ff = hidden.shape
    tokens = groups * rows
    chunks, _, piece = own.shape
    per = chunks // local
    first = group * local
    is_end = (tp == 0) | (tp == n_tp - 1)
    is_mid = (tp > 0) & (tp < n_tp - 1)
    low = tp < n_tp // 2
    near_mid = (ex, ey, jnp.where(low, 1, n_tp - 2))
    near_end = (ex, ey, jnp.where(low, 0, n_tp - 1))
    other_mid = (ex, ey, jnp.where(low, n_tp // 2, n_tp // 2 - 1))
    partner = (ex, 1 - ey, tp)

    def load(which, e):
        src = (w_down, w_gate, w_up)[which]
        dst = (wd, wg, wu)[which]
        return pltpu.make_async_copy(src.at[e], dst.at[e], w_sem.at[which * local + e])

    def save(which, e):
        src = (x_cols, scaled, hidden_t, d_gate, d_up)[which]
        dst = (x_cols_out, scaled_out, hidden_out, d_gate_out, d_up_out)[which]
        return pltpu.make_async_copy(src.at[e], dst.at[e], out_sem.at[which * local + e])

    for e in range(local):
        load(0, e).start()

    small[...] = jnp.full(small.shape, -1.0, small.dtype)
    small[:top, :rows] = gates_in[...]
    small[top : 2 * top, :rows] = ids_in[...].astype(jnp.float32).astype(jnp.bfloat16)

    bar = pltpu.get_barrier_semaphore()
    for s in range(1, n_ex):
        pl.semaphore_signal(bar, inc=1, device_id=((ex + s) % n_ex, ey, tp), device_id_type=MESH)
    pl.semaphore_signal(bar, inc=1, device_id=partner, device_id_type=MESH)

    @pl.when(is_end)
    def _():
        pl.semaphore_signal(bar, inc=1, device_id=near_mid, device_id_type=MESH)

    @pl.when(is_mid)
    def _():
        pl.semaphore_signal(bar, inc=1, device_id=near_end, device_id_type=MESH)
        pl.semaphore_signal(bar, inc=1, device_id=other_mid, device_id_type=MESH)

    with jax.named_scope("barrier"):
        @pl.when(is_end)
        def _():
            pl.semaphore_wait(bar, n_ex + 1)

        @pl.when(is_mid)
        def _():
            pl.semaphore_wait(bar, n_ex + 2)

    def remote(src, dst, send, recv, to):
        return pltpu.make_async_remote_copy(
            src_ref=src, dst_ref=dst, send_sem=send, recv_sem=recv,
            device_id=to, device_id_type=MESH,
        )

    def spread(src, dest, send, recv):
        for s in range(1, n_ex):
            to = ((ex + s) % n_ex, ey, tp)
            remote(src, dest.at[group], send.at[s - 1], recv.at[group], to).start()
        remote(src, dest.at[group], send.at[n_ex - 1], recv.at[group], partner).start()

    def relay(dest, send, recv):
        for s in range(1, n_ex):
            origin = ((ex - s + n_ex) % n_ex) * n_ey + ey
            blk = dest.at[origin]
            copy = remote(blk, blk, send.at[n_ex - 1 + s], recv.at[origin], partner)
            copy.wait_recv()
            copy.start()

    def rest(dest, send, recv):
        for c in range(n_ex):
            blk = dest.at[c * n_ey + 1 - ey]
            remote(blk, blk, send.at[0], recv.at[c * n_ey + 1 - ey], partner).wait_recv()

    def drain(src, dest, send, recv):
        for i in range(2 * n_ex - 1):
            remote(src, dest.at[group], send.at[i], recv.at[group], partner).wait_send()

    spread(small, sm_all, sm_send, sm_recv)
    spread(cot, dy_all, dy_send, dy_recv)

    def activations(e, carry):
        a = act_gate[e].astype(jnp.float32)
        u = act_up[e].astype(jnp.float32)
        q = 1.0 / (1.0 + jnp.exp(-a))
        silu = a * q
        hid = silu * u
        hidden[e] = hid.astype(jnp.bfloat16)
        hidden_t[e] = hid.T.astype(jnp.bfloat16)
        to_gate[e] = u * q * (1.0 + a * (1.0 - q))
        to_up[e] = silu
        save(2, e).start()
        return carry

    with jax.named_scope("acts"):
        sm_all[group] = small[...]
        dy_all[group] = cot[...]
        x_all[group] = tok[...]
        lax.fori_loop(0, local, activations, 0)

    with jax.named_scope("small"):
        relay(sm_all, sm_send, sm_recv)
        rest(sm_all, sm_send, sm_recv)

    with jax.named_scope("routing"):
        def lanes_of(part):
            tiles = []
            for base in range(0, tokens, LANES):
                acc = None
                for g in range(base // rows, min(groups, (base + LANES) // rows)):
                    block = sm_all[g].astype(jnp.float32)[part * top : (part + 1) * top]
                    at = g * rows - base
                    moved = pltpu.roll(block, at, axis=1) if at else block
                    lane = lax.broadcasted_iota(jnp.int32, (top, LANES), 1)
                    moved = jnp.where((lane >= at) & (lane < at + rows), moved, 0.0)
                    acc = moved if acc is None else acc + moved
                tiles.append(acc)
            return jnp.concatenate(tiles, axis=1)

        gates = lanes_of(0)
        ids = lanes_of(1)
        start = lax.broadcasted_iota(jnp.int32, (groups, rows, tokens), 0).reshape(tokens, tokens)
        at_row = lax.broadcasted_iota(jnp.int32, (tokens, tokens), 0)
        at_col = lax.broadcasted_iota(jnp.int32, (tokens, tokens), 1)
        after = (at_row < at_col) & (at_col < (start + 1) * rows)
        after = jnp.where(after, 1.0, 0.0).astype(jnp.bfloat16)
        row = lax.broadcasted_iota(jnp.int32, (top, tokens), 0)
        names = jnp.zeros((top, tokens), jnp.float32)
        named, gate_of = [], []
        for e in range(local):
            hit = ids == (first + e).astype(jnp.float32)
            named.append(jnp.sum(jnp.where(hit, 1.0, 0.0), axis=0, keepdims=True))
            gate_of.append(jnp.sum(jnp.where(hit, gates, 0.0), axis=0, keepdims=True))
            names = names + jnp.where(row == e, named[e], 0.0)
        position = mm(names.astype(jnp.bfloat16), after)
        lane = lax.broadcasted_iota(jnp.int32, (1, tokens), 1)
        base = jnp.zeros((1, tokens), jnp.int32)
        for g in range(1, groups):
            base = base + jnp.where(lane >= g * rows, cap, 0)
        base = base.astype(jnp.float32)
        slot = lax.broadcasted_iota(jnp.int32, (LANES, tokens), 0).astype(jnp.float32)
        for e in range(local):
            row_of = jnp.where(named[e] > 0.0, base + position[e : e + 1], -1.0)
            pick = jnp.where(slot == row_of, 1.0, 0.0)
            chosen[e] = pick[:slots].astype(jnp.bfloat16)
            chosen_t[e] = pick.T.astype(jnp.bfloat16)
            g_col = jnp.sum(pick[:slots] * gate_of[e], axis=1, keepdims=True)
            gate_rows[e] = jnp.broadcast_to(g_col, (slots, LANES))

    with jax.named_scope("dyrecv"):
        relay(dy_all, dy_send, dy_recv)
        for e in range(local):
            load(1, e).start()
            load(2, e).start()
        spread(tok, x_all, x_send, x_recv)
        rest(dy_all, dy_send, dy_recv)

    def to_mid(c):
        return remote(own.at[c], from_end.at[c], end_send.at[c], end_recv.at[c], near_mid)

    def to_pair(c):
        return remote(pair.at[c], from_mid.at[c], mid_send.at[c], mid_recv.at[c], other_mid)

    def to_end(c):
        return remote(total.at[c], total.at[c], tot_send.at[c], tot_recv.at[c], near_end)

    def first_pass(e, carry):
        dy = mm(chosen[e], dy_all[...].reshape(tokens, width)).astype(jnp.bfloat16)
        scaled[e] = (gate_rows[e][:, :1] * dy.astype(jnp.float32)).astype(jnp.bfloat16)
        load(0, e).wait()
        for h in range(per):
            raw = mm_dims(dy, wd[e, h * piece : (h + 1) * piece, :], NT)
            own[e * per + h] = raw.astype(jnp.bfloat16)

            @pl.when(is_end)
            def _():
                to_mid(e * per + h).start()

        save(1, e).start()
        return carry

    with jax.named_scope("first"):
        lax.fori_loop(0, local, first_pass, 0)

    def join(c):
        to_mid(c).wait_recv()
        pair[c] = (own[c].astype(jnp.float32) + from_end[c].astype(jnp.float32)).astype(jnp.bfloat16)
        to_pair(c).start()

    def arrive(c):
        @pl.when(is_mid & (c + LAG < chunks))
        def _():
            join(c + LAG)

        @pl.when(is_mid)
        def _():
            to_pair(c).wait_recv()
            both = pair[c].astype(jnp.float32) + from_mid[c].astype(jnp.float32)
            total[c] = both.astype(jnp.bfloat16)
            to_end(c).start()

        @pl.when(is_end)
        def _():
            to_end(c).wait_recv()

    with jax.named_scope("lead"):
        @pl.when(is_mid)
        def _():
            for c in range(LAG):
                join(c)

        back_acc[...] = jnp.zeros_like(back_acc)
        score_acc[...] = jnp.zeros_like(score_acc)

    def place(e, carry):
        rows_of = mm(chosen[e], x_all[...].reshape(tokens, width))
        x_cols[e] = rows_of.T.astype(jnp.bfloat16)
        save(0, e).start()
        return carry

    def second_pass(e, carry):
        for h in range(per):
            c = e * per + h
            with jax.named_scope("arrive"):
                arrive(c)

            with jax.named_scope("dx"):
                span = slice(h * piece, (h + 1) * piece)
                raw = total[c].astype(jnp.float32)
                dh = gate_rows[e][:, :1] * raw
                dg = (dh * to_gate[e, :, span]).astype(jnp.bfloat16)
                du = (dh * to_up[e, :, span]).astype(jnp.bfloat16)
                d_gate[e, :, span] = dg
                d_up[e, :, span] = du
                part = jnp.sum(raw * hidden[e, :, span].astype(jnp.float32), axis=1, keepdims=True)
                if h == 0:
                    score_cols[...] = jnp.broadcast_to(part, score_cols.shape)

                    @pl.when(e == 0)
                    def _():
                        for i in range(local):
                            load(1, i).wait()
                            load(2, i).wait()
                else:
                    score_cols[...] += part
                dx = mm_dims(dg, wg[e, :, span], NT) + mm_dims(du, wu[e, :, span], NT)
                if h == 0:
                    dx_acc[...] = dx
                else:
                    dx_acc[...] += dx
        with jax.named_scope("back"):
            save(3, e).start()
            save(4, e).start()
            pick = chosen_t[e][:, :slots]
            back_acc[...] += mm(pick, dx_acc[...].astype(jnp.bfloat16))
            at = lax.broadcasted_iota(jnp.int32, (slots, LANES), 1)
            score = jnp.where(at == e, score_cols[...], 0.0).astype(jnp.bfloat16)
            score_acc[...] += mm(pick, score)

        @pl.when(e == 0)
        def _():
            with jax.named_scope("xrelay"):
                relay(x_all, x_send, x_recv)

        @pl.when(e == 1)
        def _():
            with jax.named_scope("xplace"):
                rest(x_all, x_send, x_recv)
                lax.fori_loop(0, local, place, 0)

        return carry

    lax.fori_loop(0, local, second_pass, 0)
    with jax.named_scope("finish"):
        back[:, :, :width] = back_acc[...].astype(jnp.bfloat16).reshape(groups, rows, width)
        back[:, :, width:] = score_acc[...].astype(jnp.bfloat16).reshape(groups, rows, LANES)
        last = pltpu.make_async_copy(back, back_out, out_sem.at[5 * local])
        last.start()
        drain(small, sm_all, sm_send, sm_recv)
        drain(cot, dy_all, dy_send, dy_recv)
        drain(tok, x_all, x_send, x_recv)

        @pl.when(is_end)
        def _():
            for c in range(chunks):
                to_mid(c).wait_send()

        @pl.when(is_mid)
        def _():
            for c in range(chunks):
                to_pair(c).wait_send()
                to_end(c).wait_send()

        for which in range(5):
            for e in range(local):
                save(which, e).wait()
        last.wait()


def exchange(cap, groups, gates, ids, cot, tok, act_gate, act_up, w_gate, w_up, w_down):
    rows, width = cot.shape
    local, slots, ff = act_gate.shape
    tokens = groups * rows
    chunks = local * HALVES
    piece = ff // HALVES
    n_ex, n_ey = lax.axis_size("ex"), lax.axis_size("ey")
    bf, f32 = jnp.bfloat16, jnp.float32
    sends = 2 * n_ex - 1
    dma = pltpu.SemaphoreType.DMA
    vmem = pl.BlockSpec(memory_space=pltpu.VMEM)
    hbm = pl.BlockSpec(memory_space=pltpu.HBM)
    buf = pltpu.VMEM((chunks, slots, piece), bf)
    outs = (
        (local, width, slots), (local, slots, width), (local, ff, slots),
        (local, slots, ff), (local, slots, ff), (groups, rows, width + LANES),
    )
    return pl.pallas_call(
        functools.partial(exchange_kernel, cap),
        out_shape=tuple(jax.ShapeDtypeStruct(shape, bf) for shape in outs),
        in_specs=[vmem] * 6 + [hbm] * 3,
        out_specs=(hbm,) * 6,
        scratch_shapes=[
            pltpu.VMEM((2 * gates.shape[0], LANES), bf),
            pltpu.VMEM((groups, rows, width), bf),
            pltpu.VMEM((groups, rows, width), bf),
            pltpu.VMEM((groups, 2 * gates.shape[0], LANES), bf),
            pltpu.VMEM((local, ff, width), bf),
            pltpu.VMEM((local, width, ff), bf),
            pltpu.VMEM((local, width, ff), bf),
            pltpu.VMEM((local, slots, tokens), bf),
            pltpu.VMEM((local, tokens, LANES), bf),
            pltpu.VMEM((local, slots, LANES), f32),
            pltpu.VMEM((local, width, slots), bf),
            pltpu.VMEM((local, slots, width), bf),
            pltpu.VMEM((local, ff, slots), bf),
            pltpu.VMEM((local, slots, ff), bf),
            pltpu.VMEM((local, slots, ff), bf),
            pltpu.VMEM((local, slots, ff), bf),
            pltpu.VMEM((groups, rows, width + LANES), bf),
            pltpu.VMEM((local, slots, ff), f32),
            pltpu.VMEM((local, slots, ff), f32),
            buf, buf, buf, buf, buf,
            pltpu.VMEM((slots, width), f32),
            pltpu.VMEM((tokens, width), f32),
            pltpu.VMEM((tokens, LANES), f32),
            pltpu.VMEM((slots, LANES), f32),
            dma((3 * local,)), dma((5 * local + 1,)),
            dma((sends,)), dma((groups,)),
            dma((sends,)), dma((groups,)),
            dma((sends,)), dma((groups,)),
            dma((chunks,)), dma((chunks,)),
            dma((chunks,)), dma((chunks,)),
            dma((chunks,)), dma((chunks,)),
        ],
        compiler_params=pltpu.CompilerParams(
            collective_id=0, has_side_effects=True, vmem_limit_bytes=63 << 20
        ),
        name="exchange",
    )(gates, ids, cot, tok, act_gate, act_up, w_gate, w_up, w_down)


def weights_kernel(
    x_cols_in, scaled_in, hidden_in, d_gate_in, d_up_in,
    down_out, gate_out, up_out,
    x_cols, scaled, hidden, d_gate, d_up, down, gate, up, in_sem, out_sem,
):
    local, width, slots = x_cols.shape
    ff = hidden.shape[1]
    tile = 256
    steps = width // tile

    def load(which, e):
        src = (hidden_in, scaled_in, x_cols_in, d_gate_in, d_up_in)[which]
        dst = (hidden, scaled, x_cols, d_gate, d_up)[which]
        return pltpu.make_async_copy(src.at[e], dst.at[e], in_sem.at[which, e])

    def save(which, e, j):
        src = (down, gate, up)[which]
        dst = (down_out, gate_out, up_out)[which]
        at = pl.ds(pl.multiple_of(j * tile, tile), tile)
        index = (e, slice(None), at) if which == 0 else (e, at)
        return pltpu.make_async_copy(src.at[index], dst.at[index], out_sem.at[which, e * steps + j])

    for e in range(local):
        for which in range(5):
            load(which, e).start()

    def expert(e, carry):
        for which in range(5):
            load(which, e).wait()

        def step(j, carry):
            at = pl.ds(pl.multiple_of(j * tile, tile), tile)
            x_t = x_cols[e, at, :]
            gate[e, at, :] = mm(x_t, d_gate[e]).astype(jnp.bfloat16)
            save(1, e, j).start()
            up[e, at, :] = mm(x_t, d_up[e]).astype(jnp.bfloat16)
            save(2, e, j).start()
            down[e, :, at] = mm(hidden[e], scaled[e, :, at]).astype(jnp.bfloat16)
            save(0, e, j).start()
            return carry

        return lax.fori_loop(0, steps, step, carry)

    lax.fori_loop(0, local, expert, 0)

    def finish(e, carry):
        for which in range(3):
            for j in range(steps):
                save(which, e, j).wait()
        return carry

    lax.fori_loop(0, local, finish, 0)


def weight_grads(x_cols, scaled, hidden, d_gate, d_up):
    local, width, slots = x_cols.shape
    ff = hidden.shape[1]
    bf = jnp.bfloat16
    hbm = pl.BlockSpec(memory_space=pltpu.HBM)
    outs = ((local, ff, width), (local, width, ff), (local, width, ff))
    ins = [pltpu.VMEM(part.shape, bf) for part in (x_cols, scaled, hidden, d_gate, d_up)]
    dma = pltpu.SemaphoreType.DMA
    return pl.pallas_call(
        weights_kernel,
        out_shape=tuple(jax.ShapeDtypeStruct(shape, bf) for shape in outs),
        in_specs=[hbm] * 5,
        out_specs=(hbm,) * 3,
        scratch_shapes=ins
        + [pltpu.VMEM(shape, bf) for shape in outs]
        + [dma((5, local)), dma((3, local * (width // 256)))],
        compiler_params=pltpu.CompilerParams(vmem_limit_bytes=60 << 20),
        cost_estimate=pl.CostEstimate(
            flops=6 * local * slots * ff * width,
            bytes_accessed=6 * local * ff * width,
            transcendentals=0,
        ),
        name="weight_grads",
    )(x_cols, scaled, hidden, d_gate, d_up)


def on_device(tokens, cotangent, gates, expert_ids, saved_gate, saved_up, w_gate, w_up, w_down):
    groups = lax.axis_size(GROUP)
    rows, width = tokens.shape
    local, slots = saved_gate.shape[1:]
    act_gate = saved_gate.transpose(1, 2, 0)
    act_up = saved_up.transpose(1, 2, 0)
    x_cols, scaled, hidden, d_gate, d_up, back = exchange(
        slots // groups, groups, gates.T, expert_ids.T, cotangent, tokens,
        act_gate, act_up, w_gate, w_up, w_down,
    )
    back = lax.all_to_all(back, GROUP, split_axis=0, concat_axis=0, tiled=True)
    grad_w_down, grad_w_gate, grad_w_up = weight_grads(x_cols, scaled, hidden, d_gate, d_up)
    grad_tokens = jnp.sum(back[:, :, :width].astype(jnp.float32), axis=0).astype(jnp.bfloat16)
    table = back[:, :, width : width + local].transpose(1, 0, 2).reshape(rows, groups * local)
    picks = expert_ids[:, :, None] == jnp.arange(groups * local, dtype=jnp.int32)[None, None, :]
    grad_gates = jnp.sum(
        jnp.where(picks, table.astype(jnp.float32)[:, None, :], 0.0), axis=2
    ).astype(jnp.bfloat16)
    return (grad_tokens, grad_gates, grad_w_gate, grad_w_up, grad_w_down)


def solution(mesh):
    by_group = P(GROUP, "tp")
    small = P(GROUP, None)
    saved = P(None, GROUP, None)
    wide = P(GROUP, "tp", None)
    down = P(GROUP, None, "tp")
    in_specs = (by_group, by_group, small, small, saved, saved, wide, wide, down)
    out_specs = (by_group, small, wide, wide, down)
    fast = mesh.shape["tp"] == 4 and mesh.shape["ey"] == 2
    return jax.shard_map(
        on_device if fast else on_device_plain, mesh=mesh, in_specs=in_specs, out_specs=out_specs, check_vma=False
    )
```

```python
import functools
import jax
import jax.numpy as jnp
from jax import lax
from jax.experimental import pallas as pl
from jax.experimental.pallas import tpu as pltpu
from jax.sharding import PartitionSpec as P

LANES = 128
GROUP = ("ex", "ey")


def scatter_blocks(blocks, parts):
    if parts > 4:
        got = lax.all_to_all(blocks, "tp", split_axis=0, concat_axis=0, tiled=True)
        return [got[i] for i in range(parts)]
    me = lax.axis_index("tp")
    got = [lax.dynamic_index_in_dim(blocks, me, 0, keepdims=False)]
    for step in range(1, parts):
        piece = lax.dynamic_index_in_dim(blocks, (me + step) % parts, 0, keepdims=False)
        got.append(lax.ppermute(piece, "tp", [(i, (i + step) % parts) for i in range(parts)]))
    return got


def block_sum(terms):
    return sum(term.astype(jnp.float32) for term in terms).astype(jnp.bfloat16)


def gather_pieces(block, parts):
    if parts > 4:
        return [lax.all_gather(block, "tp", axis=0)]
    shifts = [[(i, (i + step) % parts) for i in range(parts)] for step in range(1, parts)]
    return [block] + [lax.ppermute(block, "tp", shift) for shift in shifts]


def in_order(pieces, parts):
    if parts > 4:
        return pieces[0]
    me = lax.axis_index("tp")
    whole = jnp.zeros((parts,) + pieces[0].shape, pieces[0].dtype)
    for step, piece in enumerate(pieces):
        whole = lax.dynamic_update_index_in_dim(whole, piece, (me - step) % parts, 0)
    return whole


def on_device_plain(tokens, cotangent, gates, expert_ids, saved_gate, saved_up, w_gate, w_up, w_down):
    groups = lax.axis_size(GROUP)
    parts = lax.axis_size("tp")
    rows, width = tokens.shape
    top = expert_ids.shape[1]
    hidden_units, local, slots = saved_gate.shape
    capacity = slots // groups
    total = groups * rows
    first = lax.axis_index(GROUP) * local

    extra = jnp.concatenate(
        [gates, expert_ids.astype(jnp.bfloat16), jnp.zeros((rows, LANES - 2 * top), jnp.bfloat16)],
        axis=1,
    )
    packed = jnp.concatenate([cotangent, extra], axis=1)
    packed = lax.all_gather(packed, GROUP, axis=0, tiled=True)
    tokens, packed = lax.optimization_barrier((tokens, packed))
    all_x = lax.all_to_all(
        jnp.broadcast_to(tokens[None], (groups, rows, width)),
        GROUP, split_axis=0, concat_axis=0, tiled=True,
    ).reshape(total, width)
    all_dy = packed[:, :width]
    small = packed[:, width:].astype(jnp.float32).T
    all_gates = small[:top]
    all_ids = small[top : 2 * top].astype(jnp.int32)

    match = all_ids[None] == first + jnp.arange(local, dtype=jnp.int32)[:, None, None]
    named = jnp.sum(match.astype(jnp.float32), axis=1)
    gate_of = jnp.sum(jnp.where(match, all_gates[None], 0.0), axis=1)
    place = jnp.arange(total, dtype=jnp.int32)
    group_of = place // rows
    earlier = (place[:, None] < place[None, :]) & (group_of[:, None] == group_of[None, :])
    position = jnp.dot(
        named.astype(jnp.bfloat16), earlier.astype(jnp.bfloat16), preferred_element_type=jnp.float32
    ).astype(jnp.int32)
    row_of = jnp.where(named > 0, group_of[None] * capacity + position, -1)
    taken = row_of[:, None, :] == jnp.arange(slots, dtype=jnp.int32)[None, :, None]
    chosen = taken.astype(jnp.bfloat16).reshape(local * slots, total)
    gate_rows = jnp.sum(jnp.where(taken, gate_of[:, None, :], 0.0), axis=2, keepdims=True)

    dy_rows = jnp.dot(chosen, all_dy, preferred_element_type=jnp.float32).astype(jnp.bfloat16)
    dy_rows = dy_rows.reshape(local, slots, width)
    halves = 2 if local % 2 == 0 else 1
    each = local // halves
    cuts = [slice(h * each, (h + 1) * each) for h in range(halves)]
    received = []
    for cut in cuts:
        raw = jnp.einsum(
            "erd,efd->erf", dy_rows[cut], w_down[cut], preferred_element_type=jnp.float32
        ).astype(jnp.bfloat16)
        raw = raw.reshape(parts, each * slots // parts, hidden_units)
        received.append(scatter_blocks(raw, parts))

    scaled = (gate_rows * dy_rows.astype(jnp.float32)).astype(jnp.bfloat16)
    act_gate = saved_gate.transpose(1, 2, 0).astype(jnp.float32)
    act_up = saved_up.transpose(1, 2, 0).astype(jnp.float32)
    sigm = jax.nn.sigmoid(act_gate)
    hidden = (act_gate * sigm * act_up).astype(jnp.bfloat16)
    sums = [block_sum(received[0])]
    hidden, scaled, sums[0] = lax.optimization_barrier((hidden, scaled, sums[0]))
    grad_w_down = jnp.einsum(
        "erf,erd->efd", hidden, scaled, preferred_element_type=jnp.float32
    ).astype(jnp.bfloat16)

    for terms in received[1:]:
        terms, grad_w_down = lax.optimization_barrier((terms, grad_w_down))
        sums.append(block_sum(terms))
    gathered = [gather_pieces(block, parts) for block in sums]
    d_gate, d_up, score, dx_rows = [], [], [], []
    for cut, pieces in zip(cuts, gathered):
        if dx_rows:
            pieces, dx_rows[-1] = lax.optimization_barrier((pieces, dx_rows[-1]))
        raw = in_order(pieces, parts).reshape(each, slots, hidden_units).astype(jnp.float32)
        a, u, q = act_gate[cut], act_up[cut], sigm[cut]
        dh = gate_rows[cut] * raw
        part_score = jnp.sum(raw * hidden[cut].astype(jnp.float32), axis=2, keepdims=True)
        part_gate = (dh * u * q * (1.0 + a * (1.0 - q))).astype(jnp.bfloat16)
        part_up = (dh * a * q).astype(jnp.bfloat16)
        part_gate, part_up = lax.optimization_barrier((part_gate, part_up))
        dx = jnp.einsum("erf,edf->erd", part_gate, w_gate[cut], preferred_element_type=jnp.float32)
        dx = dx + jnp.einsum("erf,edf->erd", part_up, w_up[cut], preferred_element_type=jnp.float32)
        dx_rows.append(dx.astype(jnp.bfloat16))
        d_gate.append(part_gate)
        d_up.append(part_up)
        score.append(part_score)
    d_gate, d_up, score, dx_rows = [
        jnp.concatenate(pieces, axis=0) for pieces in (d_gate, d_up, score, dx_rows)
    ]
    dx_rows = dx_rows.reshape(local * slots, width)
    own = jnp.arange(LANES)[None, None, :] == jnp.arange(local)[:, None, None]
    score_cols = jnp.where(own, score, 0.0).astype(jnp.bfloat16).reshape(local * slots, LANES)
    over_rows = (((0,), (0,)), ((), ()))
    back = [
        lax.dot_general(chosen, part, over_rows, preferred_element_type=jnp.float32).astype(
            jnp.bfloat16
        )
        for part in (dx_rows, score_cols)
    ]
    back = jnp.concatenate(back, axis=1).reshape(groups, rows, width + LANES)
    back = lax.all_to_all(back, GROUP, split_axis=0, concat_axis=0, tiled=True)

    x_rows = jnp.dot(chosen, all_x, preferred_element_type=jnp.float32).astype(jnp.bfloat16)
    x_rows = x_rows.reshape(local, slots, width)
    grad_w_gate = jnp.einsum(
        "erd,erf->edf", x_rows, d_gate, preferred_element_type=jnp.float32
    ).astype(jnp.bfloat16)
    grad_w_up = jnp.einsum(
        "erd,erf->edf", x_rows, d_up, preferred_element_type=jnp.float32
    ).astype(jnp.bfloat16)

    grad_tokens = jnp.sum(back[:, :, :width].astype(jnp.float32), axis=0).astype(jnp.bfloat16)
    table = back[:, :, width : width + local].transpose(1, 0, 2).reshape(rows, groups * local)
    picks = expert_ids[:, :, None] == jnp.arange(groups * local, dtype=jnp.int32)[None, None, :]
    grad_gates = jnp.sum(
        jnp.where(picks, table.astype(jnp.float32)[:, None, :], 0.0), axis=2
    ).astype(jnp.bfloat16)
    return (grad_tokens, grad_gates, grad_w_gate, grad_w_up, grad_w_down)


MESH = pl.DeviceIdType.MESH
SPLIT = 2
LAG = 2
STEPS = 2
NT = (((1,), (1,)), ((), ()))


def mm(a, b):
    return jnp.dot(a, b, preferred_element_type=jnp.float32)


def mm_dims(a, b, dims):
    return lax.dot_general(a, b, dims, preferred_element_type=jnp.float32)


def exchange_kernel(
    cap,
    gates_hbm, ids_hbm, cot_hbm, tok_hbm, gate_in, up_in, w_gate, w_up, w_down,
    x_cols_out, scaled_out, hidden_out, d_gate_out, d_up_out, back_out,
    small, dy_all, x_all, sm_all, wd, wg, wu, chosen, chosen_t, gate_rows,
    x_cols, scaled, hidden_t, hidden, d_gate, d_up, back, to_gate, to_up,
    own, from_end, pair, from_mid, total, dx_acc, dx_rows, score_rows, score_cols,
    dy_rows, act_gate, act_up, gates_in, ids_in, cot, tok,
    w_sem, act_sem, head_sem, out_sem, dy_send, dy_recv, x_send, x_recv, sm_send, sm_recv,
    end_send, end_recv, mid_send, mid_recv,
):
    ex, ey, tp = lax.axis_index("ex"), lax.axis_index("ey"), lax.axis_index("tp")
    n_ex, n_ey = lax.axis_size("ex"), lax.axis_size("ey")
    n_tp = lax.axis_size("tp")
    groups = n_ex * n_ey
    group = ex * n_ey + ey
    rows, width = cot.shape
    top = gates_in.shape[0]
    local, slots, ff = hidden.shape
    tokens = groups * rows
    chunks, _, piece = own.shape
    per = chunks // local
    first = group * local
    is_end = (tp == 0) | (tp == n_tp - 1)
    is_mid = (tp > 0) & (tp < n_tp - 1)
    low = tp < n_tp // 2
    near_mid = (ex, ey, jnp.where(low, 1, n_tp - 2))
    near_end = (ex, ey, jnp.where(low, 0, n_tp - 1))
    other_mid = (ex, ey, jnp.where(low, n_tp // 2, n_tp // 2 - 1))
    partner = (ex, 1 - ey, tp)

    def load(which, e):
        src = (w_down, w_gate, w_up)[which]
        dst = (wd, wg, wu)[which]
        return pltpu.make_async_copy(src.at[e], dst.at[e], w_sem.at[which])

    def loaded(which):
        src = (w_down, w_gate, w_up)[which]
        dst = (wd, wg, wu)[which]
        pltpu.make_async_copy(src, dst, w_sem.at[which]).wait()

    saves = (
        (x_cols, x_cols_out), (scaled, scaled_out), (hidden_t, hidden_out),
        (d_gate, d_gate_out), (d_up, d_up_out),
    )

    def save(which, e):
        src, dst = saves[which]
        return pltpu.make_async_copy(src.at[e], dst.at[e], out_sem.at[which])

    heads = [
        pltpu.make_async_copy(src, dst, head_sem.at[i])
        for i, (src, dst) in enumerate(
            ((gates_hbm, gates_in), (ids_hbm, ids_in), (cot_hbm, cot), (tok_hbm, tok))
        )
    ]
    for copy in heads:
        copy.start()
    in_acts = (
        pltpu.make_async_copy(gate_in, act_gate, act_sem.at[0]),
        pltpu.make_async_copy(up_in, act_up, act_sem.at[1]),
    )
    bar = pltpu.get_barrier_semaphore()
    for s in range(1, n_ex):
        pl.semaphore_signal(bar, inc=1, device_id=((ex + s) % n_ex, ey, tp), device_id_type=MESH)
    pl.semaphore_signal(bar, inc=1, device_id=partner, device_id_type=MESH)

    @pl.when(is_end)
    def _():
        pl.semaphore_signal(bar, inc=1, device_id=near_mid, device_id_type=MESH)

    @pl.when(is_mid)
    def _():
        pl.semaphore_signal(bar, inc=1, device_id=near_end, device_id_type=MESH)
        pl.semaphore_signal(bar, inc=1, device_id=other_mid, device_id_type=MESH)

    for copy in in_acts:
        copy.start()
    for e in range(local):
        load(0, e).start()
    with jax.named_scope("heads"):
        for copy in heads:
            copy.wait()
        small[...] = jnp.full(small.shape, -1.0, small.dtype)
        small[:top, :rows] = gates_in[...]
        small[top : 2 * top, :rows] = ids_in[...].astype(jnp.float32).astype(jnp.bfloat16)
        dy_all[group] = cot[...]
        x_all[group] = tok[...]

    with jax.named_scope("barrier"):
        @pl.when(is_end)
        def _():
            pl.semaphore_wait(bar, n_ex + 1)

        @pl.when(is_mid)
        def _():
            pl.semaphore_wait(bar, n_ex + 2)

    def remote(src, dst, send, recv, to):
        return pltpu.make_async_remote_copy(
            src_ref=src, dst_ref=dst, send_sem=send, recv_sem=recv,
            device_id=to, device_id_type=MESH,
        )

    def spread(src, dest, send, recv):
        mine = dest.at[group]
        for s in range(1, n_ex):
            to = ((ex + s) % n_ex, ey, tp)
            remote(src, mine, send.at[0], recv.at[s - 1], to).start()
        remote(src, mine, send.at[0], recv.at[n_ex - 1], partner).start()

    def relay(dest, send, recv):
        for s in range(1, n_ex):
            blk = dest.at[((ex - s + n_ex) % n_ex) * n_ey + ey]
            remote(blk, blk, send.at[0], recv.at[s - 1], partner).wait_recv()
            remote(blk, blk, send.at[0], recv.at[n_ex - 1], partner).start()

    def rest(dest, send, recv):
        blks = dest.at[pl.ds(0, n_ex)]
        remote(blks, blks, send.at[0], recv.at[n_ex - 1], partner).wait_recv()

    def drain(dest, send, recv):
        blks = dest.at[pl.ds(0, 2 * n_ex - 1)]
        remote(blks, blks, send.at[0], recv.at[0], partner).wait_send()

    spread(small, sm_all, sm_send, sm_recv)
    spread(cot, dy_all, dy_send, dy_recv)

    def activations(e, carry):
        a = act_gate[e].astype(jnp.float32)
        u = act_up[e].astype(jnp.float32)
        q = 1.0 / (1.0 + jnp.exp(-a))
        silu = a * q
        hid = silu * u
        hidden[e] = hid.astype(jnp.bfloat16)
        hidden_t[e] = hid.T.astype(jnp.bfloat16)
        to_gate[e] = u * q * (1.0 + a * (1.0 - q))
        to_up[e] = silu
        save(2, e).start()
        return carry

    sm_all[group] = small[...]

    with jax.named_scope("small"):
        relay(sm_all, sm_send, sm_recv)
        rest(sm_all, sm_send, sm_recv)
        for e in range(local):
            load(1, e).start()
            load(2, e).start()

    with jax.named_scope("routing"):
        def lanes_of(part):
            tiles = []
            for base in range(0, tokens, LANES):
                acc = None
                for g in range(base // rows, min(groups, (base + LANES) // rows)):
                    block = sm_all[g].astype(jnp.float32)[part * top : (part + 1) * top]
                    at = g * rows - base
                    moved = pltpu.roll(block, at, axis=1) if at else block
                    lane = lax.broadcasted_iota(jnp.int32, (top, LANES), 1)
                    moved = jnp.where((lane >= at) & (lane < at + rows), moved, 0.0)
                    acc = moved if acc is None else acc + moved
                tiles.append(acc)
            return jnp.concatenate(tiles, axis=1)

        gates = lanes_of(0)
        ids = lanes_of(1)
        start = lax.broadcasted_iota(jnp.int32, (groups, rows, tokens), 0).reshape(tokens, tokens)
        at_row = lax.broadcasted_iota(jnp.int32, (tokens, tokens), 0)
        at_col = lax.broadcasted_iota(jnp.int32, (tokens, tokens), 1)
        after = (at_row < at_col) & (at_col < (start + 1) * rows)
        after = jnp.where(after, 1.0, 0.0).astype(jnp.bfloat16)
        row = lax.broadcasted_iota(jnp.int32, (top, tokens), 0)
        names = jnp.zeros((top, tokens), jnp.float32)
        named, gate_of = [], []
        for e in range(local):
            hit = ids == (first + e).astype(jnp.float32)
            named.append(jnp.sum(jnp.where(hit, 1.0, 0.0), axis=0, keepdims=True))
            gate_of.append(jnp.sum(jnp.where(hit, gates, 0.0), axis=0, keepdims=True))
            names = names + jnp.where(row == e, named[e], 0.0)
        position = mm(names.astype(jnp.bfloat16), after)
        lane = lax.broadcasted_iota(jnp.int32, (1, tokens), 1)
        base = jnp.zeros((1, tokens), jnp.int32)
        for g in range(1, groups):
            base = base + jnp.where(lane >= g * rows, cap, 0)
        base = base.astype(jnp.float32)
        slot = lax.broadcasted_iota(jnp.int32, (LANES, tokens), 0).astype(jnp.float32)
        for e in range(local):
            row_of = jnp.where(named[e] > 0.0, base + position[e : e + 1], -1.0)
            pick = jnp.where(slot == row_of, 1.0, 0.0)
            chosen[e * slots : (e + 1) * slots] = pick[:slots].astype(jnp.bfloat16)
            g_col = jnp.sum(pick[:slots] * gate_of[e], axis=1, keepdims=True)
            gate_rows[e] = jnp.broadcast_to(g_col, (slots, LANES))
        chosen_t[...] = chosen[...].astype(jnp.float32).T.astype(jnp.bfloat16)

    with jax.named_scope("acts"):
        for copy in in_acts:
            copy.wait()
        lax.fori_loop(0, local, activations, 0)

    with jax.named_scope("dyrecv"):
        relay(dy_all, dy_send, dy_recv)
        spread(tok, x_all, x_send, x_recv)
        rest(dy_all, dy_send, dy_recv)

    def to_mid(c):
        return remote(own.at[c], from_end.at[c], end_send.at[0], end_recv.at[c], near_mid)

    def to_pair(c):
        return remote(pair.at[c], from_mid.at[c], mid_send.at[0], mid_recv.at[c], other_mid)

    def to_end(c):
        return remote(total.at[c], total.at[c], end_send.at[0], end_recv.at[c], near_end)

    def join(c):
        to_mid(c).wait_recv()
        pair[c] = (own[c].astype(jnp.float32) + from_end[c].astype(jnp.float32)).astype(jnp.bfloat16)
        to_pair(c).start()

    def pick_rows(e):
        dy = mm(chosen[e * slots : (e + 1) * slots], dy_all[...].reshape(tokens, width)).astype(jnp.bfloat16)
        dy_rows[e % 2] = dy
        scaled[e] = (gate_rows[e][:, :1] * dy.astype(jnp.float32)).astype(jnp.bfloat16)

    def first_pass(e):
        if e == local - 1:
            @pl.when(is_mid)
            def _():
                join(0)

        if e + 1 < local:
            pick_rows(e + 1)
        cuts = per if e == 0 else 1
        size = ff // cuts
        each = per // cuts
        for k in range(cuts):
            raw = mm_dims(dy_rows[e % 2], wd[e, k * size : (k + 1) * size, :], NT)
            raw = raw.astype(jnp.bfloat16)
            lo = e * per + k * each
            for h in range(each):
                own[lo + h] = raw[:, h * piece : (h + 1) * piece]

            @pl.when(is_end)
            def _():
                for h in range(each):
                    to_mid(lo + h).start()

    with jax.named_scope("first"):
        loaded(0)
        pick_rows(0)
        for e in range(local):
            first_pass(e)
            save(1, e).start()

    def arrive(c):
        @pl.when(is_mid & (c + LAG < chunks))
        def _():
            join(c + LAG)

        @pl.when(is_mid)
        def _():
            to_pair(c).wait_recv()
            both = pair[c].astype(jnp.float32) + from_mid[c].astype(jnp.float32)
            total[c] = both.astype(jnp.bfloat16)
            to_end(c).start()

        @pl.when(is_end)
        def _():
            to_end(c).wait_recv()

    with jax.named_scope("lead"):
        relay(x_all, x_send, x_recv)

        @pl.when(is_mid)
        def _():
            for c in range(1, LAG):
                join(c)

        rest(x_all, x_send, x_recv)

    def place(e):
        rows_of = mm(chosen[e * slots : (e + 1) * slots], x_all[...].reshape(tokens, width))
        x_cols[e] = rows_of.T.astype(jnp.bfloat16)
        save(0, e).start()

    with jax.named_scope("place"):
        for e in range(local):
            place(e)

    wide = ff // STEPS

    def second_pass(e, carry):
        for h in range(STEPS):
            with jax.named_scope("arrive"):
                for k in range(per // STEPS):
                    arrive(e * per + h * (per // STEPS) + k)

            with jax.named_scope("dx"):
                span = slice(h * wide, (h + 1) * wide)
                parts = [
                    total[e * per + h * (per // STEPS) + k].astype(jnp.float32)
                    for k in range(per // STEPS)
                ]
                raw = jnp.concatenate(parts, axis=1)
                dh = gate_rows[e][:, :1] * raw
                dg = (dh * to_gate[e, :, span]).astype(jnp.bfloat16)
                du = (dh * to_up[e, :, span]).astype(jnp.bfloat16)
                d_gate[e, :, span] = dg
                d_up[e, :, span] = du
                part = jnp.sum(raw * hidden[e, :, span].astype(jnp.float32), axis=1, keepdims=True)
                part = jnp.broadcast_to(part, score_cols.shape)
                if h == 0:
                    score_cols[...] = part

                    @pl.when(e == 0)
                    def _():
                        loaded(1)
                        loaded(2)
                else:
                    part = part + score_cols[...]
                    score_cols[...] = part
                dx = mm_dims(dg, wg[e, :, span], NT) + mm_dims(du, wu[e, :, span], NT)
                if h > 0:
                    dx = dx + dx_acc[...]
                if h < STEPS - 1:
                    dx_acc[...] = dx
                else:
                    dx_rows[e] = dx.astype(jnp.bfloat16)
                    at = lax.broadcasted_iota(jnp.int32, (slots, LANES), 1)
                    score_rows[e] = jnp.where(at == e, part, 0.0).astype(jnp.bfloat16)
        save(3, e).start()
        save(4, e).start()
        return carry

    lax.fori_loop(0, local, second_pass, 0)
    with jax.named_scope("back"):
        flat = dx_rows[...].reshape(local * slots, width)
        sums = mm(chosen_t[...], flat).astype(jnp.bfloat16)
        back[:, :, :width] = sums.reshape(groups, rows, width)
        flat = score_rows[...].reshape(local * slots, LANES)
        sums = mm(chosen_t[...], flat).astype(jnp.bfloat16)
        back[:, :, width:] = sums.reshape(groups, rows, LANES)
    with jax.named_scope("finish"):
        last = pltpu.make_async_copy(back, back_out, out_sem.at[5])
        last.start()
        drain(sm_all, sm_send, sm_recv)
        drain(dy_all, dy_send, dy_recv)
        drain(x_all, x_send, x_recv)

        @pl.when(is_end)
        def _():
            remote(own, from_end, end_send.at[0], end_recv.at[0], near_mid).wait_send()

        @pl.when(is_mid)
        def _():
            remote(pair, from_mid, mid_send.at[0], mid_recv.at[0], other_mid).wait_send()
            remote(total, total, end_send.at[0], end_recv.at[0], near_end).wait_send()

        for which in range(5):
            pltpu.make_async_copy(*saves[which], out_sem.at[which]).wait()
        last.wait()


def exchange(cap, groups, gates, ids, cot, tok, act_gate, act_up, w_gate, w_up, w_down):
    rows, width = cot.shape
    local, slots, ff = act_gate.shape
    tokens = groups * rows
    chunks = local * SPLIT
    piece = ff // SPLIT
    n_ex, n_ey = lax.axis_size("ex"), lax.axis_size("ey")
    bf, f32 = jnp.bfloat16, jnp.float32
    dma = pltpu.SemaphoreType.DMA
    hbm = pl.BlockSpec(memory_space=pltpu.HBM)
    buf = pltpu.VMEM((chunks, slots, piece), bf)
    outs = (
        (local, width, slots), (local, slots, width), (local, ff, slots),
        (local, slots, ff), (local, slots, ff), (groups, rows, width + LANES),
    )
    return pl.pallas_call(
        functools.partial(exchange_kernel, cap),
        out_shape=tuple(jax.ShapeDtypeStruct(shape, bf) for shape in outs),
        in_specs=[hbm] * 9,
        out_specs=(hbm,) * 6,
        scratch_shapes=[
            pltpu.VMEM((2 * gates.shape[0], LANES), bf),
            pltpu.VMEM((groups, rows, width), bf),
            pltpu.VMEM((groups, rows, width), bf),
            pltpu.VMEM((groups, 2 * gates.shape[0], LANES), bf),
            pltpu.VMEM((local, ff, width), bf),
            pltpu.VMEM((local, width, ff), bf),
            pltpu.VMEM((local, width, ff), bf),
            pltpu.VMEM((local * slots, tokens), bf),
            pltpu.VMEM((tokens, local * slots), bf),
            pltpu.VMEM((local, slots, LANES), f32),
            pltpu.VMEM((local, width, slots), bf),
            pltpu.VMEM((local, slots, width), bf),
            pltpu.VMEM((local, ff, slots), bf),
            pltpu.VMEM((local, slots, ff), bf),
            pltpu.VMEM((local, slots, ff), bf),
            pltpu.VMEM((local, slots, ff), bf),
            pltpu.VMEM((groups, rows, width + LANES), bf),
            pltpu.VMEM((local, slots, ff), f32),
            pltpu.VMEM((local, slots, ff), f32),
            buf, buf, buf, buf, buf,
            pltpu.VMEM((slots, width), f32),
            pltpu.VMEM((local, slots, width), bf),
            pltpu.VMEM((local, slots, LANES), bf),
            pltpu.VMEM((slots, LANES), f32),
            pltpu.VMEM((2, slots, width), bf),
            pltpu.VMEM((local, slots, ff), bf),
            pltpu.VMEM((local, slots, ff), bf),
            pltpu.VMEM(gates.shape, bf),
            pltpu.VMEM(ids.shape, jnp.int32),
            pltpu.VMEM((rows, width), bf),
            pltpu.VMEM((rows, width), bf),
            dma((3,)), dma((2,)), dma((4,)), dma((6,)),
            dma((1,)), dma((n_ex,)),
            dma((1,)), dma((n_ex,)),
            dma((1,)), dma((n_ex,)),
            dma((1,)), dma((chunks,)),
            dma((1,)), dma((chunks,)),
        ],
        compiler_params=pltpu.CompilerParams(
            collective_id=0, has_side_effects=True, vmem_limit_bytes=63 << 20
        ),
        name="exchange",
    )(gates, ids, cot, tok, act_gate, act_up, w_gate, w_up, w_down)


def weights_kernel(
    x_cols_in, scaled_in, hidden_in, d_gate_in, d_up_in,
    down_out, gate_out, up_out,
    x_cols, scaled, hidden, d_gate, d_up, down, gate, up, in_sem, out_sem,
):
    local, width, slots = x_cols.shape
    ff = hidden.shape[1]
    tile = 256
    steps = width // tile

    def load(which, e):
        src = (hidden_in, scaled_in, x_cols_in, d_gate_in, d_up_in)[which]
        dst = (hidden, scaled, x_cols, d_gate, d_up)[which]
        return pltpu.make_async_copy(src.at[e], dst.at[e], in_sem.at[which, e])

    def save(which, e, j):
        src = (down, gate, up)[which]
        dst = (down_out, gate_out, up_out)[which]
        at = slice(j * tile, (j + 1) * tile)
        index = (e, slice(None), at) if which == 0 else (e, at)
        return pltpu.make_async_copy(src.at[index], dst.at[index], out_sem.at[which])

    for e in range(local):
        for which in range(5):
            load(which, e).start()

    def expert(e, carry):
        for which in range(5):
            load(which, e).wait()

        for j in range(steps):
            at = slice(j * tile, (j + 1) * tile)
            x_t = x_cols[e, at, :]
            gate[e, at, :] = mm(x_t, d_gate[e]).astype(jnp.bfloat16)
            save(1, e, j).start()
            up[e, at, :] = mm(x_t, d_up[e]).astype(jnp.bfloat16)
            save(2, e, j).start()
            down[e, :, at] = mm(hidden[e], scaled[e, :, at]).astype(jnp.bfloat16)
            save(0, e, j).start()
        return carry

    lax.fori_loop(0, local, expert, 0)

    for which, (src, dst) in enumerate(((down, down_out), (gate, gate_out), (up, up_out))):
        pltpu.make_async_copy(src, dst, out_sem.at[which]).wait()


def weight_grads(x_cols, scaled, hidden, d_gate, d_up):
    local, width, slots = x_cols.shape
    ff = hidden.shape[1]
    bf = jnp.bfloat16
    hbm = pl.BlockSpec(memory_space=pltpu.HBM)
    outs = ((local, ff, width), (local, width, ff), (local, width, ff))
    ins = [pltpu.VMEM(part.shape, bf) for part in (x_cols, scaled, hidden, d_gate, d_up)]
    dma = pltpu.SemaphoreType.DMA
    return pl.pallas_call(
        weights_kernel,
        out_shape=tuple(jax.ShapeDtypeStruct(shape, bf) for shape in outs),
        in_specs=[hbm] * 5,
        out_specs=(hbm,) * 3,
        scratch_shapes=ins
        + [pltpu.VMEM(shape, bf) for shape in outs]
        + [dma((5, local)), dma((3,))],
        compiler_params=pltpu.CompilerParams(vmem_limit_bytes=60 << 20),
        cost_estimate=pl.CostEstimate(
            flops=6 * local * slots * ff * width,
            bytes_accessed=6 * local * ff * width,
            transcendentals=0,
        ),
        name="weight_grads",
    )(x_cols, scaled, hidden, d_gate, d_up)


def on_device(tokens, cotangent, gates, expert_ids, saved_gate, saved_up, w_gate, w_up, w_down):
    groups = lax.axis_size(GROUP)
    rows, width = tokens.shape
    local, slots = saved_gate.shape[1:]
    act_gate = saved_gate.transpose(1, 2, 0)
    act_up = saved_up.transpose(1, 2, 0)
    x_cols, scaled, hidden, d_gate, d_up, back = exchange(
        slots // groups, groups, gates.T, expert_ids.T, cotangent, tokens,
        act_gate, act_up, w_gate, w_up, w_down,
    )
    back = lax.all_to_all(back, GROUP, split_axis=0, concat_axis=0, tiled=True)
    grad_w_down, grad_w_gate, grad_w_up = weight_grads(x_cols, scaled, hidden, d_gate, d_up)
    grad_tokens = jnp.sum(back[:, :, :width].astype(jnp.float32), axis=0).astype(jnp.bfloat16)
    table = back[:, :, width : width + local].transpose(0, 2, 1).astype(jnp.float32)
    names = jnp.arange(groups * local, dtype=jnp.int32).reshape(groups, local, 1, 1)
    picks = expert_ids.T[None, None] == names
    grad_gates = jnp.sum(jnp.where(picks, table[:, :, None, :], 0.0), axis=(0, 1))
    grad_gates = grad_gates.astype(jnp.bfloat16).T
    return (grad_tokens, grad_gates, grad_w_gate, grad_w_up, grad_w_down)


def solution(mesh):
    by_group = P(GROUP, "tp")
    small = P(GROUP, None)
    saved = P(None, GROUP, None)
    wide = P(GROUP, "tp", None)
    down = P(GROUP, None, "tp")
    in_specs = (by_group, by_group, small, small, saved, saved, wide, wide, down)
    out_specs = (by_group, small, wide, wide, down)
    fast = mesh.shape["tp"] == 4 and mesh.shape["ey"] == 2
    return jax.shard_map(
        on_device if fast else on_device_plain, mesh=mesh, in_specs=in_specs, out_specs=out_specs, check_vma=False
    )
```

```python
import functools
import jax
import jax.numpy as jnp
from jax import lax
from jax.experimental import pallas as pl
from jax.experimental.pallas import tpu as pltpu
from jax.sharding import PartitionSpec as P

LANES = 128
GROUP = ("ex", "ey")


def scatter_blocks(blocks, parts):
    if parts > 4:
        got = lax.all_to_all(blocks, "tp", split_axis=0, concat_axis=0, tiled=True)
        return [got[i] for i in range(parts)]
    me = lax.axis_index("tp")
    got = [lax.dynamic_index_in_dim(blocks, me, 0, keepdims=False)]
    for step in range(1, parts):
        piece = lax.dynamic_index_in_dim(blocks, (me + step) % parts, 0, keepdims=False)
        got.append(lax.ppermute(piece, "tp", [(i, (i + step) % parts) for i in range(parts)]))
    return got


def block_sum(terms):
    return sum(term.astype(jnp.float32) for term in terms).astype(jnp.bfloat16)


def gather_pieces(block, parts):
    if parts > 4:
        return [lax.all_gather(block, "tp", axis=0)]
    shifts = [[(i, (i + step) % parts) for i in range(parts)] for step in range(1, parts)]
    return [block] + [lax.ppermute(block, "tp", shift) for shift in shifts]


def in_order(pieces, parts):
    if parts > 4:
        return pieces[0]
    me = lax.axis_index("tp")
    whole = jnp.zeros((parts,) + pieces[0].shape, pieces[0].dtype)
    for step, piece in enumerate(pieces):
        whole = lax.dynamic_update_index_in_dim(whole, piece, (me - step) % parts, 0)
    return whole


def on_device_plain(tokens, cotangent, gates, expert_ids, saved_gate, saved_up, w_gate, w_up, w_down):
    groups = lax.axis_size(GROUP)
    parts = lax.axis_size("tp")
    rows, width = tokens.shape
    top = expert_ids.shape[1]
    hidden_units, local, slots = saved_gate.shape
    capacity = slots // groups
    total = groups * rows
    first = lax.axis_index(GROUP) * local

    extra = jnp.concatenate(
        [gates, expert_ids.astype(jnp.bfloat16), jnp.zeros((rows, LANES - 2 * top), jnp.bfloat16)],
        axis=1,
    )
    packed = jnp.concatenate([cotangent, extra], axis=1)
    packed = lax.all_gather(packed, GROUP, axis=0, tiled=True)
    tokens, packed = lax.optimization_barrier((tokens, packed))
    all_x = lax.all_to_all(
        jnp.broadcast_to(tokens[None], (groups, rows, width)),
        GROUP, split_axis=0, concat_axis=0, tiled=True,
    ).reshape(total, width)
    all_dy = packed[:, :width]
    small = packed[:, width:].astype(jnp.float32).T
    all_gates = small[:top]
    all_ids = small[top : 2 * top].astype(jnp.int32)

    match = all_ids[None] == first + jnp.arange(local, dtype=jnp.int32)[:, None, None]
    named = jnp.sum(match.astype(jnp.float32), axis=1)
    gate_of = jnp.sum(jnp.where(match, all_gates[None], 0.0), axis=1)
    place = jnp.arange(total, dtype=jnp.int32)
    group_of = place // rows
    earlier = (place[:, None] < place[None, :]) & (group_of[:, None] == group_of[None, :])
    position = jnp.dot(
        named.astype(jnp.bfloat16), earlier.astype(jnp.bfloat16), preferred_element_type=jnp.float32
    ).astype(jnp.int32)
    row_of = jnp.where(named > 0, group_of[None] * capacity + position, -1)
    taken = row_of[:, None, :] == jnp.arange(slots, dtype=jnp.int32)[None, :, None]
    chosen = taken.astype(jnp.bfloat16).reshape(local * slots, total)
    gate_rows = jnp.sum(jnp.where(taken, gate_of[:, None, :], 0.0), axis=2, keepdims=True)

    dy_rows = jnp.dot(chosen, all_dy, preferred_element_type=jnp.float32).astype(jnp.bfloat16)
    dy_rows = dy_rows.reshape(local, slots, width)
    halves = 2 if local % 2 == 0 else 1
    each = local // halves
    cuts = [slice(h * each, (h + 1) * each) for h in range(halves)]
    received = []
    for cut in cuts:
        raw = jnp.einsum(
            "erd,efd->erf", dy_rows[cut], w_down[cut], preferred_element_type=jnp.float32
        ).astype(jnp.bfloat16)
        raw = raw.reshape(parts, each * slots // parts, hidden_units)
        received.append(scatter_blocks(raw, parts))

    scaled = (gate_rows * dy_rows.astype(jnp.float32)).astype(jnp.bfloat16)
    act_gate = saved_gate.transpose(1, 2, 0).astype(jnp.float32)
    act_up = saved_up.transpose(1, 2, 0).astype(jnp.float32)
    sigm = jax.nn.sigmoid(act_gate)
    hidden = (act_gate * sigm * act_up).astype(jnp.bfloat16)
    sums = [block_sum(received[0])]
    hidden, scaled, sums[0] = lax.optimization_barrier((hidden, scaled, sums[0]))
    grad_w_down = jnp.einsum(
        "erf,erd->efd", hidden, scaled, preferred_element_type=jnp.float32
    ).astype(jnp.bfloat16)

    for terms in received[1:]:
        terms, grad_w_down = lax.optimization_barrier((terms, grad_w_down))
        sums.append(block_sum(terms))
    gathered = [gather_pieces(block, parts) for block in sums]
    d_gate, d_up, score, dx_rows = [], [], [], []
    for cut, pieces in zip(cuts, gathered):
        if dx_rows:
            pieces, dx_rows[-1] = lax.optimization_barrier((pieces, dx_rows[-1]))
        raw = in_order(pieces, parts).reshape(each, slots, hidden_units).astype(jnp.float32)
        a, u, q = act_gate[cut], act_up[cut], sigm[cut]
        dh = gate_rows[cut] * raw
        part_score = jnp.sum(raw * hidden[cut].astype(jnp.float32), axis=2, keepdims=True)
        part_gate = (dh * u * q * (1.0 + a * (1.0 - q))).astype(jnp.bfloat16)
        part_up = (dh * a * q).astype(jnp.bfloat16)
        part_gate, part_up = lax.optimization_barrier((part_gate, part_up))
        dx = jnp.einsum("erf,edf->erd", part_gate, w_gate[cut], preferred_element_type=jnp.float32)
        dx = dx + jnp.einsum("erf,edf->erd", part_up, w_up[cut], preferred_element_type=jnp.float32)
        dx_rows.append(dx.astype(jnp.bfloat16))
        d_gate.append(part_gate)
        d_up.append(part_up)
        score.append(part_score)
    d_gate, d_up, score, dx_rows = [
        jnp.concatenate(pieces, axis=0) for pieces in (d_gate, d_up, score, dx_rows)
    ]
    dx_rows = dx_rows.reshape(local * slots, width)
    own = jnp.arange(LANES)[None, None, :] == jnp.arange(local)[:, None, None]
    score_cols = jnp.where(own, score, 0.0).astype(jnp.bfloat16).reshape(local * slots, LANES)
    over_rows = (((0,), (0,)), ((), ()))
    back = [
        lax.dot_general(chosen, part, over_rows, preferred_element_type=jnp.float32).astype(
            jnp.bfloat16
        )
        for part in (dx_rows, score_cols)
    ]
    back = jnp.concatenate(back, axis=1).reshape(groups, rows, width + LANES)
    back = lax.all_to_all(back, GROUP, split_axis=0, concat_axis=0, tiled=True)

    x_rows = jnp.dot(chosen, all_x, preferred_element_type=jnp.float32).astype(jnp.bfloat16)
    x_rows = x_rows.reshape(local, slots, width)
    grad_w_gate = jnp.einsum(
        "erd,erf->edf", x_rows, d_gate, preferred_element_type=jnp.float32
    ).astype(jnp.bfloat16)
    grad_w_up = jnp.einsum(
        "erd,erf->edf", x_rows, d_up, preferred_element_type=jnp.float32
    ).astype(jnp.bfloat16)

    grad_tokens = jnp.sum(back[:, :, :width].astype(jnp.float32), axis=0).astype(jnp.bfloat16)
    table = back[:, :, width : width + local].transpose(1, 0, 2).reshape(rows, groups * local)
    picks = expert_ids[:, :, None] == jnp.arange(groups * local, dtype=jnp.int32)[None, None, :]
    grad_gates = jnp.sum(
        jnp.where(picks, table.astype(jnp.float32)[:, None, :], 0.0), axis=2
    ).astype(jnp.bfloat16)
    return (grad_tokens, grad_gates, grad_w_gate, grad_w_up, grad_w_down)


MESH = pl.DeviceIdType.MESH
SPLIT = 2
LAG = 2
STEPS = 2
NT = (((1,), (1,)), ((), ()))


def mm(a, b):
    return jnp.dot(a, b, preferred_element_type=jnp.float32)


def mm_dims(a, b, dims):
    return lax.dot_general(a, b, dims, preferred_element_type=jnp.float32)


def exchange_kernel(
    cap,
    gates_hbm, ids_hbm, cot_hbm, tok_hbm, gate_in, up_in, w_gate, w_up, w_down,
    x_out, scaled_out, hidden, d_gate, d_up, back,
    small, dy_all, x_all, sm_all, wd, wg, wu, chosen, chosen_t, gate_rows,
    x_rows, scaled, to_gate, to_up,
    own, from_end, pair, from_mid, total, dx_acc, dx_rows, score_rows, score_cols,
    dy_rows, act_gate, act_up, gates_in, ids_in, cot, tok,
    w_sem, act_sem, head_sem, out_sem, dy_send, dy_recv, x_send, x_recv, sm_send, sm_recv,
    end_send, end_recv, mid_send, mid_recv,
):
    ex, ey, tp = lax.axis_index("ex"), lax.axis_index("ey"), lax.axis_index("tp")
    n_ex, n_ey = lax.axis_size("ex"), lax.axis_size("ey")
    n_tp = lax.axis_size("tp")
    groups = n_ex * n_ey
    group = ex * n_ey + ey
    rows, width = cot.shape
    top = gates_in.shape[0]
    local, slots, ff = hidden.shape
    tokens = groups * rows
    chunks, _, piece = own.shape
    per = chunks // local
    first = group * local
    is_end = (tp == 0) | (tp == n_tp - 1)
    is_mid = (tp > 0) & (tp < n_tp - 1)
    low = tp < n_tp // 2
    near_mid = (ex, ey, jnp.where(low, 1, n_tp - 2))
    near_end = (ex, ey, jnp.where(low, 0, n_tp - 1))
    other_mid = (ex, ey, jnp.where(low, n_tp // 2, n_tp // 2 - 1))
    partner = (ex, 1 - ey, tp)

    def load(which, e):
        src = (w_down, w_gate, w_up)[which]
        dst = (wd, wg, wu)[which]
        return pltpu.make_async_copy(src.at[e], dst.at[e], w_sem.at[which])

    def loaded(which):
        src = (w_down, w_gate, w_up)[which]
        dst = (wd, wg, wu)[which]
        pltpu.make_async_copy(src, dst, w_sem.at[which]).wait()

    saves = ((scaled, scaled_out), (x_rows, x_out))

    def save(which, e):
        src, dst = saves[which]
        return pltpu.make_async_copy(src.at[e], dst.at[e], out_sem.at[which])

    heads = [
        pltpu.make_async_copy(src, dst, head_sem.at[i])
        for i, (src, dst) in enumerate(
            ((gates_hbm, gates_in), (ids_hbm, ids_in), (cot_hbm, cot), (tok_hbm, tok))
        )
    ]
    for copy in heads:
        copy.start()
    in_acts = (
        pltpu.make_async_copy(gate_in, act_gate, act_sem.at[0]),
        pltpu.make_async_copy(up_in, act_up, act_sem.at[1]),
    )
    bar = pltpu.get_barrier_semaphore()
    for s in range(1, n_ex):
        pl.semaphore_signal(bar, inc=1, device_id=((ex + s) % n_ex, ey, tp), device_id_type=MESH)
    pl.semaphore_signal(bar, inc=1, device_id=partner, device_id_type=MESH)

    @pl.when(is_end)
    def _():
        pl.semaphore_signal(bar, inc=1, device_id=near_mid, device_id_type=MESH)

    @pl.when(is_mid)
    def _():
        pl.semaphore_signal(bar, inc=1, device_id=near_end, device_id_type=MESH)
        pl.semaphore_signal(bar, inc=1, device_id=other_mid, device_id_type=MESH)

    for copy in in_acts:
        copy.start()
    for e in range(local):
        load(0, e).start()
    with jax.named_scope("heads"):
        for copy in heads:
            copy.wait()
        small[...] = jnp.full(small.shape, -1.0, small.dtype)
        small[:top, :rows] = gates_in[...]
        small[top : 2 * top, :rows] = ids_in[...].astype(jnp.float32).astype(jnp.bfloat16)
        dy_all[group] = cot[...]
        x_all[group] = tok[...]

    with jax.named_scope("barrier"):
        @pl.when(is_end)
        def _():
            pl.semaphore_wait(bar, n_ex + 1)

        @pl.when(is_mid)
        def _():
            pl.semaphore_wait(bar, n_ex + 2)

    def remote(src, dst, send, recv, to):
        return pltpu.make_async_remote_copy(
            src_ref=src, dst_ref=dst, send_sem=send, recv_sem=recv,
            device_id=to, device_id_type=MESH,
        )

    def spread(src, dest, send, recv):
        mine = dest.at[group]
        for s in range(1, n_ex):
            to = ((ex + s) % n_ex, ey, tp)
            remote(src, mine, send.at[0], recv.at[s - 1], to).start()
        remote(src, mine, send.at[0], recv.at[n_ex - 1], partner).start()

    def relay(dest, send, recv):
        for s in range(1, n_ex):
            blk = dest.at[((ex - s + n_ex) % n_ex) * n_ey + ey]
            remote(blk, blk, send.at[0], recv.at[s - 1], partner).wait_recv()
            remote(blk, blk, send.at[0], recv.at[n_ex - 1], partner).start()

    def rest(dest, send, recv):
        blks = dest.at[pl.ds(0, n_ex)]
        remote(blks, blks, send.at[0], recv.at[n_ex - 1], partner).wait_recv()

    def drain(dest, send, recv):
        blks = dest.at[pl.ds(0, 2 * n_ex - 1)]
        remote(blks, blks, send.at[0], recv.at[0], partner).wait_send()

    spread(small, sm_all, sm_send, sm_recv)
    spread(cot, dy_all, dy_send, dy_recv)

    def activations(e, carry):
        a = act_gate[e].astype(jnp.float32)
        u = act_up[e].astype(jnp.float32)
        q = 1.0 / (1.0 + jnp.exp(-a))
        silu = a * q
        hid = silu * u
        hidden[e] = hid.astype(jnp.bfloat16)
        to_gate[e] = u * q * (1.0 + a * (1.0 - q))
        to_up[e] = silu
        return carry

    sm_all[group] = small[...]

    with jax.named_scope("small"):
        relay(sm_all, sm_send, sm_recv)
        rest(sm_all, sm_send, sm_recv)
        for e in range(local):
            load(1, e).start()
            load(2, e).start()

    with jax.named_scope("routing"):
        def lanes_of(part):
            tiles = []
            for base in range(0, tokens, LANES):
                acc = None
                for g in range(base // rows, min(groups, (base + LANES) // rows)):
                    block = sm_all[g].astype(jnp.float32)[part * top : (part + 1) * top]
                    at = g * rows - base
                    moved = pltpu.roll(block, at, axis=1) if at else block
                    lane = lax.broadcasted_iota(jnp.int32, (top, LANES), 1)
                    moved = jnp.where((lane >= at) & (lane < at + rows), moved, 0.0)
                    acc = moved if acc is None else acc + moved
                tiles.append(acc)
            return jnp.concatenate(tiles, axis=1)

        gates = lanes_of(0)
        ids = lanes_of(1)
        start = lax.broadcasted_iota(jnp.int32, (groups, rows, tokens), 0).reshape(tokens, tokens)
        at_row = lax.broadcasted_iota(jnp.int32, (tokens, tokens), 0)
        at_col = lax.broadcasted_iota(jnp.int32, (tokens, tokens), 1)
        after = (at_row < at_col) & (at_col < (start + 1) * rows)
        after = jnp.where(after, 1.0, 0.0).astype(jnp.bfloat16)
        row = lax.broadcasted_iota(jnp.int32, (top, tokens), 0)
        names = jnp.zeros((top, tokens), jnp.float32)
        named, gate_of = [], []
        for e in range(local):
            hit = ids == (first + e).astype(jnp.float32)
            named.append(jnp.sum(jnp.where(hit, 1.0, 0.0), axis=0, keepdims=True))
            gate_of.append(jnp.sum(jnp.where(hit, gates, 0.0), axis=0, keepdims=True))
            names = names + jnp.where(row == e, named[e], 0.0)
        position = mm(names.astype(jnp.bfloat16), after)
        lane = lax.broadcasted_iota(jnp.int32, (1, tokens), 1)
        base = jnp.zeros((1, tokens), jnp.int32)
        for g in range(1, groups):
            base = base + jnp.where(lane >= g * rows, cap, 0)
        base = base.astype(jnp.float32)
        slot = lax.broadcasted_iota(jnp.int32, (LANES, tokens), 0).astype(jnp.float32)
        for e in range(local):
            row_of = jnp.where(named[e] > 0.0, base + position[e : e + 1], -1.0)
            pick = jnp.where(slot == row_of, 1.0, 0.0)
            chosen[e * slots : (e + 1) * slots] = pick[:slots].astype(jnp.bfloat16)
            g_col = jnp.sum(pick[:slots] * gate_of[e], axis=1, keepdims=True)
            gate_rows[e] = jnp.broadcast_to(g_col, (slots, LANES))
        chosen_t[...] = chosen[...].astype(jnp.float32).T.astype(jnp.bfloat16)

    with jax.named_scope("acts"):
        for copy in in_acts:
            copy.wait()
        lax.fori_loop(0, local, activations, 0)

    with jax.named_scope("dyrecv"):
        relay(dy_all, dy_send, dy_recv)
        spread(tok, x_all, x_send, x_recv)
        rest(dy_all, dy_send, dy_recv)

    def to_mid(c):
        return remote(own.at[c], from_end.at[c], end_send.at[0], end_recv.at[c], near_mid)

    def to_pair(c):
        return remote(pair.at[c], from_mid.at[c], mid_send.at[0], mid_recv.at[c], other_mid)

    def to_end(c):
        return remote(total.at[c], total.at[c], end_send.at[0], end_recv.at[c], near_end)

    def join(c):
        to_mid(c).wait_recv()
        pair[c] = (own[c].astype(jnp.float32) + from_end[c].astype(jnp.float32)).astype(jnp.bfloat16)
        to_pair(c).start()

    def pick_rows(e):
        dy = mm(chosen[e * slots : (e + 1) * slots], dy_all[...].reshape(tokens, width)).astype(jnp.bfloat16)
        dy_rows[e % 2] = dy
        scaled[e] = (gate_rows[e][:, :1] * dy.astype(jnp.float32)).astype(jnp.bfloat16)

    def first_pass(e):
        if e == local - 1:
            @pl.when(is_mid)
            def _():
                join(0)

        if e + 1 < local:
            pick_rows(e + 1)
        cuts = per if e == 0 else 1
        size = ff // cuts
        each = per // cuts
        for k in range(cuts):
            raw = mm_dims(dy_rows[e % 2], wd[e, k * size : (k + 1) * size, :], NT)
            raw = raw.astype(jnp.bfloat16)
            lo = e * per + k * each
            for h in range(each):
                own[lo + h] = raw[:, h * piece : (h + 1) * piece]

            @pl.when(is_end)
            def _():
                for h in range(each):
                    to_mid(lo + h).start()

    with jax.named_scope("first"):
        loaded(0)
        pick_rows(0)
        for e in range(local):
            first_pass(e)
            save(0, e).start()

    def arrive(c):
        @pl.when(is_mid & (c + LAG < chunks))
        def _():
            join(c + LAG)

        @pl.when(is_mid)
        def _():
            to_pair(c).wait_recv()
            both = pair[c].astype(jnp.float32) + from_mid[c].astype(jnp.float32)
            total[c] = both.astype(jnp.bfloat16)
            to_end(c).start()

        @pl.when(is_end)
        def _():
            to_end(c).wait_recv()

    with jax.named_scope("lead"):
        relay(x_all, x_send, x_recv)

        @pl.when(is_mid)
        def _():
            for c in range(1, LAG):
                join(c)

        rest(x_all, x_send, x_recv)

    def place(e):
        rows_of = mm(chosen[e * slots : (e + 1) * slots], x_all[...].reshape(tokens, width))
        x_rows[e] = rows_of.astype(jnp.bfloat16)
        save(1, e).start()

    with jax.named_scope("place"):
        for e in range(local):
            place(e)

    wide = ff // STEPS

    def second_pass(e, carry):
        for h in range(STEPS):
            with jax.named_scope("arrive"):
                for k in range(per // STEPS):
                    arrive(e * per + h * (per // STEPS) + k)

            with jax.named_scope("dx"):
                span = slice(h * wide, (h + 1) * wide)
                parts = [
                    total[e * per + h * (per // STEPS) + k].astype(jnp.float32)
                    for k in range(per // STEPS)
                ]
                raw = jnp.concatenate(parts, axis=1)
                dh = gate_rows[e][:, :1] * raw
                dg = (dh * to_gate[e, :, span]).astype(jnp.bfloat16)
                du = (dh * to_up[e, :, span]).astype(jnp.bfloat16)
                d_gate[e, :, span] = dg
                d_up[e, :, span] = du
                part = jnp.sum(raw * hidden[e, :, span].astype(jnp.float32), axis=1, keepdims=True)
                part = jnp.broadcast_to(part, score_cols.shape)
                if h == 0:
                    score_cols[...] = part

                    @pl.when(e == 0)
                    def _():
                        loaded(1)
                        loaded(2)
                else:
                    part = part + score_cols[...]
                    score_cols[...] = part
                dx = mm_dims(dg, wg[e, :, span], NT) + mm_dims(du, wu[e, :, span], NT)
                if h > 0:
                    dx = dx + dx_acc[...]
                if h < STEPS - 1:
                    dx_acc[...] = dx
                else:
                    dx_rows[e] = dx.astype(jnp.bfloat16)
                    at = lax.broadcasted_iota(jnp.int32, (slots, LANES), 1)
                    score_rows[e] = jnp.where(at == e, part, 0.0).astype(jnp.bfloat16)
        return carry

    lax.fori_loop(0, local, second_pass, 0)
    with jax.named_scope("back"):
        flat = dx_rows[...].reshape(local * slots, width)
        sums = mm(chosen_t[...], flat).astype(jnp.bfloat16)
        back[:, :, :width] = sums.reshape(groups, rows, width)
        flat = score_rows[...].reshape(local * slots, LANES)
        sums = mm(chosen_t[...], flat).astype(jnp.bfloat16)
        back[:, :, width:] = sums.reshape(groups, rows, LANES)
    with jax.named_scope("finish"):
        for which in range(2):
            pltpu.make_async_copy(*saves[which], out_sem.at[which]).wait()
        drain(sm_all, sm_send, sm_recv)
        drain(dy_all, dy_send, dy_recv)
        drain(x_all, x_send, x_recv)

        @pl.when(is_end)
        def _():
            remote(own, from_end, end_send.at[0], end_recv.at[0], near_mid).wait_send()

        @pl.when(is_mid)
        def _():
            remote(pair, from_mid, mid_send.at[0], mid_recv.at[0], other_mid).wait_send()
            remote(total, total, end_send.at[0], end_recv.at[0], near_end).wait_send()


def exchange(cap, groups, gates, ids, cot, tok, act_gate, act_up, w_gate, w_up, w_down):
    rows, width = cot.shape
    local, slots, ff = act_gate.shape
    tokens = groups * rows
    chunks = local * SPLIT
    piece = ff // SPLIT
    n_ex, n_ey = lax.axis_size("ex"), lax.axis_size("ey")
    bf, f32 = jnp.bfloat16, jnp.float32
    dma = pltpu.SemaphoreType.DMA
    hbm = pl.BlockSpec(memory_space=pltpu.HBM)
    buf = pltpu.VMEM((chunks, slots, piece), bf)
    vmem = pl.BlockSpec(memory_space=pltpu.VMEM)
    outs = (
        (local, slots, width), (local, slots, width), (local, slots, ff),
        (local, slots, ff), (local, slots, ff), (groups, rows, width + LANES),
    )
    kept = [
        pltpu.VMEM(shape, bf) if 2 <= i < 5 else jax.ShapeDtypeStruct(shape, bf)
        for i, shape in enumerate(outs)
    ]
    return pl.pallas_call(
        functools.partial(exchange_kernel, cap),
        out_shape=tuple(kept),
        in_specs=[hbm] * 9,
        out_specs=(hbm, hbm, vmem, vmem, vmem, vmem),
        scratch_shapes=[
            pltpu.VMEM((2 * gates.shape[0], LANES), bf),
            pltpu.VMEM((groups, rows, width), bf),
            pltpu.VMEM((groups, rows, width), bf),
            pltpu.VMEM((groups, 2 * gates.shape[0], LANES), bf),
            pltpu.VMEM((local, ff, width), bf),
            pltpu.VMEM((local, width, ff), bf),
            pltpu.VMEM((local, width, ff), bf),
            pltpu.VMEM((local * slots, tokens), bf),
            pltpu.VMEM((tokens, local * slots), bf),
            pltpu.VMEM((local, slots, LANES), f32),
            pltpu.VMEM((local, slots, width), bf),
            pltpu.VMEM((local, slots, width), bf),
            pltpu.VMEM((local, slots, ff), f32),
            pltpu.VMEM((local, slots, ff), f32),
            buf, buf, buf, buf, buf,
            pltpu.VMEM((slots, width), f32),
            pltpu.VMEM((local, slots, width), bf),
            pltpu.VMEM((local, slots, LANES), bf),
            pltpu.VMEM((slots, LANES), f32),
            pltpu.VMEM((2, slots, width), bf),
            pltpu.VMEM((local, slots, ff), bf),
            pltpu.VMEM((local, slots, ff), bf),
            pltpu.VMEM(gates.shape, bf),
            pltpu.VMEM(ids.shape, jnp.int32),
            pltpu.VMEM((rows, width), bf),
            pltpu.VMEM((rows, width), bf),
            dma((3,)), dma((2,)), dma((4,)), dma((2,)),
            dma((1,)), dma((n_ex,)),
            dma((1,)), dma((n_ex,)),
            dma((1,)), dma((n_ex,)),
            dma((1,)), dma((chunks,)),
            dma((1,)), dma((chunks,)),
        ],
        compiler_params=pltpu.CompilerParams(
            collective_id=0, has_side_effects=True, vmem_limit_bytes=60 << 20
        ),
        name="exchange",
    )(gates, ids, cot, tok, act_gate, act_up, w_gate, w_up, w_down)


def weights_kernel(
    x_in, scaled_in, hidden, d_gate, d_up,
    down_out, gate_out, up_out, x_rows, scaled, x_cols, hid_cols, down, gate, up, in_sem, out_sem,
):
    local, slots, width = x_rows.shape
    tile = 256
    steps = width // tile

    def save(which, e, j):
        src = (down, gate, up)[which]
        dst = (down_out, gate_out, up_out)[which]
        at = slice(j * tile, (j + 1) * tile)
        index = (e, slice(None), at) if which == 0 else (e, at)
        return pltpu.make_async_copy(src.at[index], dst.at[index], out_sem.at[which])

    def load(which, e):
        src = (scaled_in, x_in)[which]
        dst = (scaled, x_rows)[which]
        return pltpu.make_async_copy(src.at[e], dst.at[e], in_sem.at[which, e])

    for e in range(local):
        for which in range(2):
            load(which, e).start()

    def flip(e):
        hid_cols[...] = hidden[e].astype(jnp.float32).T.astype(jnp.bfloat16)
        load(0, e).wait()
        load(1, e).wait()
        x_cols[...] = x_rows[e].astype(jnp.float32).T.astype(jnp.bfloat16)

    def expert(e, carry):
        flip(e)
        for j in range(steps):
            at = slice(j * tile, (j + 1) * tile)
            x_t = x_cols[at, :]
            gate[e, at, :] = mm(x_t, d_gate[e]).astype(jnp.bfloat16)
            save(1, e, j).start()
            up[e, at, :] = mm(x_t, d_up[e]).astype(jnp.bfloat16)
            save(2, e, j).start()
            down[e, :, at] = mm(hid_cols[...], scaled[e, :, at]).astype(jnp.bfloat16)
            save(0, e, j).start()
        return carry

    lax.fori_loop(0, local, expert, 0)
    for which, (src, dst) in enumerate(((down, down_out), (gate, gate_out), (up, up_out))):
        pltpu.make_async_copy(src, dst, out_sem.at[which]).wait()


def weight_grads(x_rows, scaled, hidden, d_gate, d_up):
    local, slots, width = x_rows.shape
    ff = hidden.shape[2]
    bf = jnp.bfloat16
    hbm = pl.BlockSpec(memory_space=pltpu.HBM)
    vmem = pl.BlockSpec(memory_space=pltpu.VMEM)
    outs = ((local, ff, width), (local, width, ff), (local, width, ff))
    return pl.pallas_call(
        weights_kernel,
        out_shape=tuple(jax.ShapeDtypeStruct(shape, bf) for shape in outs),
        in_specs=[hbm, hbm, vmem, vmem, vmem],
        out_specs=(hbm,) * 3,
        scratch_shapes=[pltpu.VMEM(scaled.shape, bf), pltpu.VMEM(scaled.shape, bf), pltpu.VMEM((width, slots), bf), pltpu.VMEM((ff, slots), bf)]
        + [pltpu.VMEM(shape, bf) for shape in outs]
        + [pltpu.SemaphoreType.DMA((2, local)), pltpu.SemaphoreType.DMA((3,))],
        compiler_params=pltpu.CompilerParams(vmem_limit_bytes=52 << 20),
        cost_estimate=pl.CostEstimate(
            flops=6 * local * slots * ff * width,
            bytes_accessed=6 * local * ff * width,
            transcendentals=0,
        ),
        name="weight_grads",
    )(x_rows, scaled, hidden, d_gate, d_up)


def on_device(tokens, cotangent, gates, expert_ids, saved_gate, saved_up, w_gate, w_up, w_down):
    groups = lax.axis_size(GROUP)
    rows, width = tokens.shape
    local, slots = saved_gate.shape[1:]
    act_gate = saved_gate.transpose(1, 2, 0)
    act_up = saved_up.transpose(1, 2, 0)
    x_rows, scaled, hidden, d_gate, d_up, back = exchange(
        slots // groups, groups, gates.T, expert_ids.T, cotangent, tokens,
        act_gate, act_up, w_gate, w_up, w_down,
    )
    back = lax.all_to_all(back, GROUP, split_axis=0, concat_axis=0, tiled=True)
    grad_w_down, grad_w_gate, grad_w_up = weight_grads(x_rows, scaled, hidden, d_gate, d_up)
    grad_tokens = jnp.sum(back[:, :, :width].astype(jnp.float32), axis=0).astype(jnp.bfloat16)
    table = back[:, :, width : width + local].transpose(0, 2, 1).astype(jnp.float32)
    names = jnp.arange(groups * local, dtype=jnp.int32).reshape(groups, local, 1, 1)
    picks = expert_ids.T[None, None] == names
    grad_gates = jnp.sum(jnp.where(picks, table[:, :, None, :], 0.0), axis=(0, 1))
    grad_gates = grad_gates.astype(jnp.bfloat16).T
    return (grad_tokens, grad_gates, grad_w_gate, grad_w_up, grad_w_down)


def solution(mesh):
    by_group = P(GROUP, "tp")
    small = P(GROUP, None)
    saved = P(None, GROUP, None)
    wide = P(GROUP, "tp", None)
    down = P(GROUP, None, "tp")
    in_specs = (by_group, by_group, small, small, saved, saved, wide, wide, down)
    out_specs = (by_group, small, wide, wide, down)
    fast = mesh.shape["tp"] == 4 and mesh.shape["ey"] == 2
    return jax.shard_map(
        on_device if fast else on_device_plain, mesh=mesh, in_specs=in_specs, out_specs=out_specs, check_vma=False
    )
```

```python
import functools
import jax
import jax.numpy as jnp
from jax import lax
from jax.experimental import pallas as pl
from jax.experimental.pallas import tpu as pltpu
from jax.sharding import PartitionSpec as P

LANES = 128
GROUP = ("ex", "ey")


def scatter_blocks(blocks, parts):
    if parts > 4:
        got = lax.all_to_all(blocks, "tp", split_axis=0, concat_axis=0, tiled=True)
        return [got[i] for i in range(parts)]
    me = lax.axis_index("tp")
    got = [lax.dynamic_index_in_dim(blocks, me, 0, keepdims=False)]
    for step in range(1, parts):
        piece = lax.dynamic_index_in_dim(blocks, (me + step) % parts, 0, keepdims=False)
        got.append(lax.ppermute(piece, "tp", [(i, (i + step) % parts) for i in range(parts)]))
    return got


def block_sum(terms):
    return sum(term.astype(jnp.float32) for term in terms).astype(jnp.bfloat16)


def gather_pieces(block, parts):
    if parts > 4:
        return [lax.all_gather(block, "tp", axis=0)]
    shifts = [[(i, (i + step) % parts) for i in range(parts)] for step in range(1, parts)]
    return [block] + [lax.ppermute(block, "tp", shift) for shift in shifts]


def in_order(pieces, parts):
    if parts > 4:
        return pieces[0]
    me = lax.axis_index("tp")
    whole = jnp.zeros((parts,) + pieces[0].shape, pieces[0].dtype)
    for step, piece in enumerate(pieces):
        whole = lax.dynamic_update_index_in_dim(whole, piece, (me - step) % parts, 0)
    return whole


def on_device_plain(tokens, cotangent, gates, expert_ids, saved_gate, saved_up, w_gate, w_up, w_down):
    groups = lax.axis_size(GROUP)
    parts = lax.axis_size("tp")
    rows, width = tokens.shape
    top = expert_ids.shape[1]
    hidden_units, local, slots = saved_gate.shape
    capacity = slots // groups
    total = groups * rows
    first = lax.axis_index(GROUP) * local

    extra = jnp.concatenate(
        [gates, expert_ids.astype(jnp.bfloat16), jnp.zeros((rows, LANES - 2 * top), jnp.bfloat16)],
        axis=1,
    )
    packed = jnp.concatenate([cotangent, extra], axis=1)
    packed = lax.all_gather(packed, GROUP, axis=0, tiled=True)
    tokens, packed = lax.optimization_barrier((tokens, packed))
    all_x = lax.all_to_all(
        jnp.broadcast_to(tokens[None], (groups, rows, width)),
        GROUP, split_axis=0, concat_axis=0, tiled=True,
    ).reshape(total, width)
    all_dy = packed[:, :width]
    small = packed[:, width:].astype(jnp.float32).T
    all_gates = small[:top]
    all_ids = small[top : 2 * top].astype(jnp.int32)

    match = all_ids[None] == first + jnp.arange(local, dtype=jnp.int32)[:, None, None]
    named = jnp.sum(match.astype(jnp.float32), axis=1)
    gate_of = jnp.sum(jnp.where(match, all_gates[None], 0.0), axis=1)
    place = jnp.arange(total, dtype=jnp.int32)
    group_of = place // rows
    earlier = (place[:, None] < place[None, :]) & (group_of[:, None] == group_of[None, :])
    position = jnp.dot(
        named.astype(jnp.bfloat16), earlier.astype(jnp.bfloat16), preferred_element_type=jnp.float32
    ).astype(jnp.int32)
    row_of = jnp.where(named > 0, group_of[None] * capacity + position, -1)
    taken = row_of[:, None, :] == jnp.arange(slots, dtype=jnp.int32)[None, :, None]
    chosen = taken.astype(jnp.bfloat16).reshape(local * slots, total)
    gate_rows = jnp.sum(jnp.where(taken, gate_of[:, None, :], 0.0), axis=2, keepdims=True)

    dy_rows = jnp.dot(chosen, all_dy, preferred_element_type=jnp.float32).astype(jnp.bfloat16)
    dy_rows = dy_rows.reshape(local, slots, width)
    halves = 2 if local % 2 == 0 else 1
    each = local // halves
    cuts = [slice(h * each, (h + 1) * each) for h in range(halves)]
    received = []
    for cut in cuts:
        raw = jnp.einsum(
            "erd,efd->erf", dy_rows[cut], w_down[cut], preferred_element_type=jnp.float32
        ).astype(jnp.bfloat16)
        raw = raw.reshape(parts, each * slots // parts, hidden_units)
        received.append(scatter_blocks(raw, parts))

    scaled = (gate_rows * dy_rows.astype(jnp.float32)).astype(jnp.bfloat16)
    act_gate = saved_gate.transpose(1, 2, 0).astype(jnp.float32)
    act_up = saved_up.transpose(1, 2, 0).astype(jnp.float32)
    sigm = jax.nn.sigmoid(act_gate)
    hidden = (act_gate * sigm * act_up).astype(jnp.bfloat16)
    sums = [block_sum(received[0])]
    hidden, scaled, sums[0] = lax.optimization_barrier((hidden, scaled, sums[0]))
    grad_w_down = jnp.einsum(
        "erf,erd->efd", hidden, scaled, preferred_element_type=jnp.float32
    ).astype(jnp.bfloat16)

    for terms in received[1:]:
        terms, grad_w_down = lax.optimization_barrier((terms, grad_w_down))
        sums.append(block_sum(terms))
    gathered = [gather_pieces(block, parts) for block in sums]
    d_gate, d_up, score, dx_rows = [], [], [], []
    for cut, pieces in zip(cuts, gathered):
        if dx_rows:
            pieces, dx_rows[-1] = lax.optimization_barrier((pieces, dx_rows[-1]))
        raw = in_order(pieces, parts).reshape(each, slots, hidden_units).astype(jnp.float32)
        a, u, q = act_gate[cut], act_up[cut], sigm[cut]
        dh = gate_rows[cut] * raw
        part_score = jnp.sum(raw * hidden[cut].astype(jnp.float32), axis=2, keepdims=True)
        part_gate = (dh * u * q * (1.0 + a * (1.0 - q))).astype(jnp.bfloat16)
        part_up = (dh * a * q).astype(jnp.bfloat16)
        part_gate, part_up = lax.optimization_barrier((part_gate, part_up))
        dx = jnp.einsum("erf,edf->erd", part_gate, w_gate[cut], preferred_element_type=jnp.float32)
        dx = dx + jnp.einsum("erf,edf->erd", part_up, w_up[cut], preferred_element_type=jnp.float32)
        dx_rows.append(dx.astype(jnp.bfloat16))
        d_gate.append(part_gate)
        d_up.append(part_up)
        score.append(part_score)
    d_gate, d_up, score, dx_rows = [
        jnp.concatenate(pieces, axis=0) for pieces in (d_gate, d_up, score, dx_rows)
    ]
    dx_rows = dx_rows.reshape(local * slots, width)
    own = jnp.arange(LANES)[None, None, :] == jnp.arange(local)[:, None, None]
    score_cols = jnp.where(own, score, 0.0).astype(jnp.bfloat16).reshape(local * slots, LANES)
    over_rows = (((0,), (0,)), ((), ()))
    back = [
        lax.dot_general(chosen, part, over_rows, preferred_element_type=jnp.float32).astype(
            jnp.bfloat16
        )
        for part in (dx_rows, score_cols)
    ]
    back = jnp.concatenate(back, axis=1).reshape(groups, rows, width + LANES)
    back = lax.all_to_all(back, GROUP, split_axis=0, concat_axis=0, tiled=True)

    x_rows = jnp.dot(chosen, all_x, preferred_element_type=jnp.float32).astype(jnp.bfloat16)
    x_rows = x_rows.reshape(local, slots, width)
    grad_w_gate = jnp.einsum(
        "erd,erf->edf", x_rows, d_gate, preferred_element_type=jnp.float32
    ).astype(jnp.bfloat16)
    grad_w_up = jnp.einsum(
        "erd,erf->edf", x_rows, d_up, preferred_element_type=jnp.float32
    ).astype(jnp.bfloat16)

    grad_tokens = jnp.sum(back[:, :, :width].astype(jnp.float32), axis=0).astype(jnp.bfloat16)
    table = back[:, :, width : width + local].transpose(1, 0, 2).reshape(rows, groups * local)
    picks = expert_ids[:, :, None] == jnp.arange(groups * local, dtype=jnp.int32)[None, None, :]
    grad_gates = jnp.sum(
        jnp.where(picks, table.astype(jnp.float32)[:, None, :], 0.0), axis=2
    ).astype(jnp.bfloat16)
    return (grad_tokens, grad_gates, grad_w_gate, grad_w_up, grad_w_down)


MESH = pl.DeviceIdType.MESH
SPLIT = 2
LAG = 2
STEPS = 2
NT = (((1,), (1,)), ((), ()))


def mm(a, b):
    return jnp.dot(a, b, preferred_element_type=jnp.float32)


def mm_dims(a, b, dims):
    return lax.dot_general(a, b, dims, preferred_element_type=jnp.float32)


def exchange_kernel(
    cap,
    gates_hbm, ids_hbm, cot_hbm, tok_hbm, gate_in, up_in, w_gate, w_up, w_down,
    x_out, scaled_out, hidden, d_gate, d_up, back_out,
    small, dy_all, x_all, sm_all, wd, wg, wu, chosen, chosen_t, gate_rows,
    x_rows, scaled, back, to_gate, to_up,
    own, from_end, pair, from_mid, total, dx_acc, dx_rows, score_rows, score_cols,
    dy_rows, act_gate, act_up, gates_in, ids_in, cot, tok,
    w_sem, act_sem, head_sem, out_sem, dy_send, dy_recv, x_send, x_recv, sm_send, sm_recv,
    end_send, end_recv, mid_send, mid_recv,
):
    ex, ey, tp = lax.axis_index("ex"), lax.axis_index("ey"), lax.axis_index("tp")
    n_ex, n_ey = lax.axis_size("ex"), lax.axis_size("ey")
    n_tp = lax.axis_size("tp")
    groups = n_ex * n_ey
    group = ex * n_ey + ey
    rows, width = cot.shape
    top = gates_in.shape[0]
    local, slots, ff = hidden.shape
    tokens = groups * rows
    chunks, _, piece = own.shape
    per = chunks // local
    first = group * local
    is_end = (tp == 0) | (tp == n_tp - 1)
    is_mid = (tp > 0) & (tp < n_tp - 1)
    low = tp < n_tp // 2
    near_mid = (ex, ey, jnp.where(low, 1, n_tp - 2))
    near_end = (ex, ey, jnp.where(low, 0, n_tp - 1))
    other_mid = (ex, ey, jnp.where(low, n_tp // 2, n_tp // 2 - 1))
    partner = (ex, 1 - ey, tp)

    def load(which, e):
        src = (w_down, w_gate, w_up)[which]
        dst = (wd, wg, wu)[which]
        return pltpu.make_async_copy(src.at[e], dst.at[e], w_sem.at[which])

    def loaded(which):
        src = (w_down, w_gate, w_up)[which]
        dst = (wd, wg, wu)[which]
        pltpu.make_async_copy(src, dst, w_sem.at[which]).wait()

    saves = ((scaled, scaled_out), (x_rows, x_out))

    def save(which, e):
        src, dst = saves[which]
        return pltpu.make_async_copy(src.at[e], dst.at[e], out_sem.at[which])

    heads = [
        pltpu.make_async_copy(src, dst, head_sem.at[i])
        for i, (src, dst) in enumerate(
            ((gates_hbm, gates_in), (ids_hbm, ids_in), (cot_hbm, cot), (tok_hbm, tok))
        )
    ]
    for copy in heads:
        copy.start()
    in_acts = (
        pltpu.make_async_copy(gate_in, act_gate, act_sem.at[0]),
        pltpu.make_async_copy(up_in, act_up, act_sem.at[1]),
    )
    bar = pltpu.get_barrier_semaphore()
    for s in range(1, n_ex):
        pl.semaphore_signal(bar, inc=1, device_id=((ex + s) % n_ex, ey, tp), device_id_type=MESH)
    pl.semaphore_signal(bar, inc=1, device_id=partner, device_id_type=MESH)

    @pl.when(is_end)
    def _():
        pl.semaphore_signal(bar, inc=1, device_id=near_mid, device_id_type=MESH)

    @pl.when(is_mid)
    def _():
        pl.semaphore_signal(bar, inc=1, device_id=near_end, device_id_type=MESH)
        pl.semaphore_signal(bar, inc=1, device_id=other_mid, device_id_type=MESH)

    for copy in in_acts:
        copy.start()
    for e in range(local):
        load(0, e).start()
    with jax.named_scope("heads"):
        for copy in heads:
            copy.wait()
        small[...] = jnp.full(small.shape, -1.0, small.dtype)
        small[:top, :rows] = gates_in[...]
        small[top : 2 * top, :rows] = ids_in[...].astype(jnp.float32).astype(jnp.bfloat16)
        dy_all[group] = cot[...]
        x_all[group] = tok[...]

    with jax.named_scope("barrier"):
        @pl.when(is_end)
        def _():
            pl.semaphore_wait(bar, n_ex + 1)

        @pl.when(is_mid)
        def _():
            pl.semaphore_wait(bar, n_ex + 2)

    def remote(src, dst, send, recv, to):
        return pltpu.make_async_remote_copy(
            src_ref=src, dst_ref=dst, send_sem=send, recv_sem=recv,
            device_id=to, device_id_type=MESH,
        )

    def spread(src, dest, send, recv):
        mine = dest.at[group]
        for s in range(1, n_ex):
            to = ((ex + s) % n_ex, ey, tp)
            remote(src, mine, send.at[0], recv.at[s - 1], to).start()
        remote(src, mine, send.at[0], recv.at[n_ex - 1], partner).start()

    def relay(dest, send, recv):
        for s in range(1, n_ex):
            blk = dest.at[((ex - s + n_ex) % n_ex) * n_ey + ey]
            remote(blk, blk, send.at[0], recv.at[s - 1], partner).wait_recv()
            remote(blk, blk, send.at[0], recv.at[n_ex - 1], partner).start()

    def rest(dest, send, recv):
        blks = dest.at[pl.ds(0, n_ex)]
        remote(blks, blks, send.at[0], recv.at[n_ex - 1], partner).wait_recv()

    def drain(dest, send, recv):
        blks = dest.at[pl.ds(0, 2 * n_ex - 1)]
        remote(blks, blks, send.at[0], recv.at[0], partner).wait_send()

    spread(small, sm_all, sm_send, sm_recv)
    spread(cot, dy_all, dy_send, dy_recv)

    def activations(e, carry):
        a = act_gate[e].astype(jnp.float32)
        u = act_up[e].astype(jnp.float32)
        q = 1.0 / (1.0 + jnp.exp(-a))
        silu = a * q
        hid = silu * u
        hidden[e] = hid.astype(jnp.bfloat16)
        to_gate[e] = u * q * (1.0 + a * (1.0 - q))
        to_up[e] = silu
        return carry

    sm_all[group] = small[...]

    with jax.named_scope("small"):
        relay(sm_all, sm_send, sm_recv)
        rest(sm_all, sm_send, sm_recv)
        for e in range(local):
            load(1, e).start()
            load(2, e).start()

    with jax.named_scope("routing"):
        def lanes_of(part):
            tiles = []
            for base in range(0, tokens, LANES):
                acc = None
                for g in range(base // rows, min(groups, (base + LANES) // rows)):
                    block = sm_all[g].astype(jnp.float32)[part * top : (part + 1) * top]
                    at = g * rows - base
                    moved = pltpu.roll(block, at, axis=1) if at else block
                    lane = lax.broadcasted_iota(jnp.int32, (top, LANES), 1)
                    moved = jnp.where((lane >= at) & (lane < at + rows), moved, 0.0)
                    acc = moved if acc is None else acc + moved
                tiles.append(acc)
            return jnp.concatenate(tiles, axis=1)

        gates = lanes_of(0)
        ids = lanes_of(1)
        start = lax.broadcasted_iota(jnp.int32, (groups, rows, tokens), 0).reshape(tokens, tokens)
        at_row = lax.broadcasted_iota(jnp.int32, (tokens, tokens), 0)
        at_col = lax.broadcasted_iota(jnp.int32, (tokens, tokens), 1)
        after = (at_row < at_col) & (at_col < (start + 1) * rows)
        after = jnp.where(after, 1.0, 0.0).astype(jnp.bfloat16)
        row = lax.broadcasted_iota(jnp.int32, (top, tokens), 0)
        names = jnp.zeros((top, tokens), jnp.float32)
        named, gate_of = [], []
        for e in range(local):
            hit = ids == (first + e).astype(jnp.float32)
            named.append(jnp.sum(jnp.where(hit, 1.0, 0.0), axis=0, keepdims=True))
            gate_of.append(jnp.sum(jnp.where(hit, gates, 0.0), axis=0, keepdims=True))
            names = names + jnp.where(row == e, named[e], 0.0)
        position = mm(names.astype(jnp.bfloat16), after)
        lane = lax.broadcasted_iota(jnp.int32, (1, tokens), 1)
        base = jnp.zeros((1, tokens), jnp.int32)
        for g in range(1, groups):
            base = base + jnp.where(lane >= g * rows, cap, 0)
        base = base.astype(jnp.float32)
        slot = lax.broadcasted_iota(jnp.int32, (LANES, tokens), 0).astype(jnp.float32)
        for e in range(local):
            row_of = jnp.where(named[e] > 0.0, base + position[e : e + 1], -1.0)
            pick = jnp.where(slot == row_of, 1.0, 0.0)
            chosen[e * slots : (e + 1) * slots] = pick[:slots].astype(jnp.bfloat16)
            g_col = jnp.sum(pick[:slots] * gate_of[e], axis=1, keepdims=True)
            gate_rows[e] = jnp.broadcast_to(g_col, (slots, LANES))
        chosen_t[...] = chosen[...].astype(jnp.float32).T.astype(jnp.bfloat16)

    with jax.named_scope("acts"):
        for copy in in_acts:
            copy.wait()
        lax.fori_loop(0, local, activations, 0)

    with jax.named_scope("dyrecv"):
        relay(dy_all, dy_send, dy_recv)
        spread(tok, x_all, x_send, x_recv)
        rest(dy_all, dy_send, dy_recv)

    def to_mid(c):
        return remote(own.at[c], from_end.at[c], end_send.at[0], end_recv.at[c], near_mid)

    def to_pair(c):
        return remote(pair.at[c], from_mid.at[c], mid_send.at[0], mid_recv.at[c], other_mid)

    def to_end(c):
        return remote(total.at[c], total.at[c], end_send.at[0], end_recv.at[c], near_end)

    def join(c):
        to_mid(c).wait_recv()
        pair[c] = (own[c].astype(jnp.float32) + from_end[c].astype(jnp.float32)).astype(jnp.bfloat16)
        to_pair(c).start()

    def pick_rows(e):
        dy = mm(chosen[e * slots : (e + 1) * slots], dy_all[...].reshape(tokens, width)).astype(jnp.bfloat16)
        dy_rows[e % 2] = dy
        scaled[e] = (gate_rows[e][:, :1] * dy.astype(jnp.float32)).astype(jnp.bfloat16)

    def first_pass(e):
        if e == local - 1:
            @pl.when(is_mid)
            def _():
                join(0)

        if e + 1 < local:
            pick_rows(e + 1)
        cuts = per if e == 0 else 1
        size = ff // cuts
        each = per // cuts
        for k in range(cuts):
            raw = mm_dims(dy_rows[e % 2], wd[e, k * size : (k + 1) * size, :], NT)
            raw = raw.astype(jnp.bfloat16)
            lo = e * per + k * each
            for h in range(each):
                own[lo + h] = raw[:, h * piece : (h + 1) * piece]

            @pl.when(is_end)
            def _():
                for h in range(each):
                    to_mid(lo + h).start()

    with jax.named_scope("first"):
        loaded(0)
        pick_rows(0)
        for e in range(local):
            first_pass(e)
            save(0, e).start()

    def arrive(c):
        @pl.when(is_mid & (c + LAG < chunks))
        def _():
            join(c + LAG)

        @pl.when(is_mid)
        def _():
            to_pair(c).wait_recv()
            both = pair[c].astype(jnp.float32) + from_mid[c].astype(jnp.float32)
            total[c] = both.astype(jnp.bfloat16)
            to_end(c).start()

        @pl.when(is_end)
        def _():
            to_end(c).wait_recv()

    with jax.named_scope("lead"):
        relay(x_all, x_send, x_recv)

        @pl.when(is_mid)
        def _():
            for c in range(1, LAG):
                join(c)

        rest(x_all, x_send, x_recv)

    def place(e):
        rows_of = mm(chosen[e * slots : (e + 1) * slots], x_all[...].reshape(tokens, width))
        x_rows[e] = rows_of.astype(jnp.bfloat16)
        save(1, e).start()

    with jax.named_scope("place"):
        for e in range(local):
            place(e)

    wide = ff // STEPS

    def second_pass(e, carry):
        for h in range(STEPS):
            with jax.named_scope("arrive"):
                for k in range(per // STEPS):
                    arrive(e * per + h * (per // STEPS) + k)

            with jax.named_scope("dx"):
                span = slice(h * wide, (h + 1) * wide)
                parts = [
                    total[e * per + h * (per // STEPS) + k].astype(jnp.float32)
                    for k in range(per // STEPS)
                ]
                raw = jnp.concatenate(parts, axis=1)
                dh = gate_rows[e][:, :1] * raw
                dg = (dh * to_gate[e, :, span]).astype(jnp.bfloat16)
                du = (dh * to_up[e, :, span]).astype(jnp.bfloat16)
                d_gate[e, :, span] = dg
                d_up[e, :, span] = du
                part = jnp.sum(raw * hidden[e, :, span].astype(jnp.float32), axis=1, keepdims=True)
                part = jnp.broadcast_to(part, score_cols.shape)
                if h == 0:
                    score_cols[...] = part

                    @pl.when(e == 0)
                    def _():
                        loaded(1)
                        loaded(2)
                else:
                    part = part + score_cols[...]
                    score_cols[...] = part
                dx = mm_dims(dg, wg[e, :, span], NT) + mm_dims(du, wu[e, :, span], NT)
                if h > 0:
                    dx = dx + dx_acc[...]
                if h < STEPS - 1:
                    dx_acc[...] = dx
                else:
                    dx_rows[e] = dx.astype(jnp.bfloat16)
                    at = lax.broadcasted_iota(jnp.int32, (slots, LANES), 1)
                    score_rows[e] = jnp.where(at == e, part, 0.0).astype(jnp.bfloat16)
        return carry

    lax.fori_loop(0, local, second_pass, 0)
    with jax.named_scope("back"):
        middle = width // 2 // LANES * LANES
        bounds = (width, width + LANES), (0, middle), (middle, width)
        sent = []
        for n, (lo, hi) in enumerate(bounds):
            source = score_rows[...] if lo == width else dx_rows[:, :, lo:hi]
            flat = source.reshape(local * slots, hi - lo)
            sums = mm(chosen_t[...], flat).astype(jnp.bfloat16)
            back[:, :, lo:hi] = sums.reshape(groups, rows, hi - lo)
            part = (slice(None), slice(None), slice(lo, hi))
            sent.append(pltpu.make_async_copy(back.at[part], back_out.at[part], out_sem.at[2 + n]))
            sent[-1].start()
    with jax.named_scope("finish"):
        for which in range(2):
            pltpu.make_async_copy(*saves[which], out_sem.at[which]).wait()
        drain(sm_all, sm_send, sm_recv)
        drain(dy_all, dy_send, dy_recv)
        drain(x_all, x_send, x_recv)

        @pl.when(is_end)
        def _():
            remote(own, from_end, end_send.at[0], end_recv.at[0], near_mid).wait_send()

        @pl.when(is_mid)
        def _():
            remote(pair, from_mid, mid_send.at[0], mid_recv.at[0], other_mid).wait_send()
            remote(total, total, end_send.at[0], end_recv.at[0], near_end).wait_send()

        for copy in sent:
            copy.wait()


def exchange(cap, groups, gates, ids, cot, tok, act_gate, act_up, w_gate, w_up, w_down):
    rows, width = cot.shape
    local, slots, ff = act_gate.shape
    tokens = groups * rows
    chunks = local * SPLIT
    piece = ff // SPLIT
    n_ex, n_ey = lax.axis_size("ex"), lax.axis_size("ey")
    bf, f32 = jnp.bfloat16, jnp.float32
    dma = pltpu.SemaphoreType.DMA
    hbm = pl.BlockSpec(memory_space=pltpu.HBM)
    buf = pltpu.VMEM((chunks, slots, piece), bf)
    vmem = pl.BlockSpec(memory_space=pltpu.VMEM)
    outs = (
        (local, slots, width), (local, slots, width), (local, slots, ff),
        (local, slots, ff), (local, slots, ff), (groups, rows, width + LANES),
    )
    kept = [
        pltpu.VMEM(shape, bf) if 2 <= i < 5 else jax.ShapeDtypeStruct(shape, bf)
        for i, shape in enumerate(outs)
    ]
    return pl.pallas_call(
        functools.partial(exchange_kernel, cap),
        out_shape=tuple(kept),
        in_specs=[hbm] * 9,
        out_specs=(hbm, hbm, vmem, vmem, vmem, hbm),
        scratch_shapes=[
            pltpu.VMEM((2 * gates.shape[0], LANES), bf),
            pltpu.VMEM((groups, rows, width), bf),
            pltpu.VMEM((groups, rows, width), bf),
            pltpu.VMEM((groups, 2 * gates.shape[0], LANES), bf),
            pltpu.VMEM((local, ff, width), bf),
            pltpu.VMEM((local, width, ff), bf),
            pltpu.VMEM((local, width, ff), bf),
            pltpu.VMEM((local * slots, tokens), bf),
            pltpu.VMEM((tokens, local * slots), bf),
            pltpu.VMEM((local, slots, LANES), f32),
            pltpu.VMEM((local, slots, width), bf),
            pltpu.VMEM((local, slots, width), bf),
            pltpu.VMEM((groups, rows, width + LANES), bf),
            pltpu.VMEM((local, slots, ff), f32),
            pltpu.VMEM((local, slots, ff), f32),
            buf, buf, buf, buf, buf,
            pltpu.VMEM((slots, width), f32),
            pltpu.VMEM((local, slots, width), bf),
            pltpu.VMEM((local, slots, LANES), bf),
            pltpu.VMEM((slots, LANES), f32),
            pltpu.VMEM((2, slots, width), bf),
            pltpu.VMEM((local, slots, ff), bf),
            pltpu.VMEM((local, slots, ff), bf),
            pltpu.VMEM(gates.shape, bf),
            pltpu.VMEM(ids.shape, jnp.int32),
            pltpu.VMEM((rows, width), bf),
            pltpu.VMEM((rows, width), bf),
            dma((3,)), dma((2,)), dma((4,)), dma((5,)),
            dma((1,)), dma((n_ex,)),
            dma((1,)), dma((n_ex,)),
            dma((1,)), dma((n_ex,)),
            dma((1,)), dma((chunks,)),
            dma((1,)), dma((chunks,)),
        ],
        compiler_params=pltpu.CompilerParams(
            collective_id=0, has_side_effects=True, vmem_limit_bytes=60 << 20
        ),
        name="exchange",
    )(gates, ids, cot, tok, act_gate, act_up, w_gate, w_up, w_down)


def weights_kernel(
    x_in, scaled_in, hidden, d_gate, d_up,
    down_out, gate_out, up_out, x_rows, scaled, x_cols, hid_cols, down, gate, up, in_sem, out_sem,
):
    local, slots, width = x_rows.shape
    tile = 256
    steps = width // tile

    def save(which, e, j):
        src = (down, gate, up)[which]
        dst = (down_out, gate_out, up_out)[which]
        at = slice(j * tile, (j + 1) * tile)
        index = (e, slice(None), at) if which == 0 else (e, at)
        return pltpu.make_async_copy(src.at[index], dst.at[index], out_sem.at[which])

    def load(which, e):
        src = (scaled_in, x_in)[which]
        dst = (scaled, x_rows)[which]
        return pltpu.make_async_copy(src.at[e], dst.at[e], in_sem.at[which, e])

    for e in range(local):
        for which in range(2):
            load(which, e).start()

    def flip(e):
        hid_cols[...] = hidden[e].astype(jnp.float32).T.astype(jnp.bfloat16)
        load(0, e).wait()
        load(1, e).wait()
        x_cols[...] = x_rows[e].astype(jnp.float32).T.astype(jnp.bfloat16)

    def expert(e, carry):
        flip(e)
        for j in range(steps):
            at = slice(j * tile, (j + 1) * tile)
            x_t = x_cols[at, :]
            gate[e, at, :] = mm(x_t, d_gate[e]).astype(jnp.bfloat16)
            save(1, e, j).start()
            up[e, at, :] = mm(x_t, d_up[e]).astype(jnp.bfloat16)
            save(2, e, j).start()
            down[e, :, at] = mm(hid_cols[...], scaled[e, :, at]).astype(jnp.bfloat16)
            save(0, e, j).start()
        return carry

    lax.fori_loop(0, local, expert, 0)
    for which, (src, dst) in enumerate(((down, down_out), (gate, gate_out), (up, up_out))):
        pltpu.make_async_copy(src, dst, out_sem.at[which]).wait()


def weight_grads(x_rows, scaled, hidden, d_gate, d_up):
    local, slots, width = x_rows.shape
    ff = hidden.shape[2]
    bf = jnp.bfloat16
    hbm = pl.BlockSpec(memory_space=pltpu.HBM)
    vmem = pl.BlockSpec(memory_space=pltpu.VMEM)
    outs = ((local, ff, width), (local, width, ff), (local, width, ff))
    return pl.pallas_call(
        weights_kernel,
        out_shape=tuple(jax.ShapeDtypeStruct(shape, bf) for shape in outs),
        in_specs=[hbm, hbm, vmem, vmem, vmem],
        out_specs=(hbm,) * 3,
        scratch_shapes=[pltpu.VMEM(scaled.shape, bf), pltpu.VMEM(scaled.shape, bf), pltpu.VMEM((width, slots), bf), pltpu.VMEM((ff, slots), bf)]
        + [pltpu.VMEM(shape, bf) for shape in outs]
        + [pltpu.SemaphoreType.DMA((2, local)), pltpu.SemaphoreType.DMA((3,))],
        compiler_params=pltpu.CompilerParams(vmem_limit_bytes=52 << 20),
        cost_estimate=pl.CostEstimate(
            flops=6 * local * slots * ff * width,
            bytes_accessed=6 * local * ff * width,
            transcendentals=0,
        ),
        name="weight_grads",
    )(x_rows, scaled, hidden, d_gate, d_up)


def on_device(tokens, cotangent, gates, expert_ids, saved_gate, saved_up, w_gate, w_up, w_down):
    groups = lax.axis_size(GROUP)
    rows, width = tokens.shape
    local, slots = saved_gate.shape[1:]
    act_gate = saved_gate.transpose(1, 2, 0)
    act_up = saved_up.transpose(1, 2, 0)
    x_rows, scaled, hidden, d_gate, d_up, back = exchange(
        slots // groups, groups, gates.T, expert_ids.T, cotangent, tokens,
        act_gate, act_up, w_gate, w_up, w_down,
    )
    back = lax.all_to_all(back, GROUP, split_axis=0, concat_axis=0, tiled=True)
    grad_w_down, grad_w_gate, grad_w_up = weight_grads(x_rows, scaled, hidden, d_gate, d_up)
    grad_tokens = jnp.sum(back[:, :, :width].astype(jnp.float32), axis=0).astype(jnp.bfloat16)
    table = back[:, :, width : width + local].transpose(0, 2, 1).astype(jnp.float32)
    names = jnp.arange(groups * local, dtype=jnp.int32).reshape(groups, local, 1, 1)
    picks = expert_ids.T[None, None] == names
    grad_gates = jnp.sum(jnp.where(picks, table[:, :, None, :], 0.0), axis=(0, 1))
    grad_gates = grad_gates.astype(jnp.bfloat16).T
    return (grad_tokens, grad_gates, grad_w_gate, grad_w_up, grad_w_down)


def solution(mesh):
    by_group = P(GROUP, "tp")
    small = P(GROUP, None)
    saved = P(None, GROUP, None)
    wide = P(GROUP, "tp", None)
    down = P(GROUP, None, "tp")
    in_specs = (by_group, by_group, small, small, saved, saved, wide, wide, down)
    out_specs = (by_group, small, wide, wide, down)
    fast = mesh.shape["tp"] == 4 and mesh.shape["ey"] == 2
    return jax.shard_map(
        on_device if fast else on_device_plain, mesh=mesh, in_specs=in_specs, out_specs=out_specs, check_vma=False
    )
```
